32 devices in a mesh: gx: 2 (over x), gy: 16 (over z, y, core).
Axes of the slice: x: 2, y: 2, z: 4, core: 2. Of those that a mesh axis runs over, the one named last changes fastest.
Arguments:
- cell: int32 [1048576], P(('gx', 'gy')), may hold values from 0 to 524287
- vehicle: int32 [1048576], P(('gx', 'gy')), may hold values from 0 to 1023
- speed: float32 [1048576], P(('gx', 'gy')), may hold values from 0 to 64, as said below
Outputs:
- top_speed: float32 [524288], P(('gx', 'gy'))
- top_vehicle: int32 [524288], P(('gx', 'gy'))
The draws below stay inside these ranges and needn't reach their ends.
Inputs may be any that keep to these rules, and one draw needn't show every extreme that they name: Every speed is a whole multiple of 1/1024.
All inputs are finite; a program needn't handle non-finite values.
Results may differ from the reference program's by a relative error of at most 0.0003.
Values sent between devices are 32-bit elements; how exact they have to be, the bound alone decides.
No kernel may reach another device: no remote copies, remote signals or barrier semaphores. Data moves between devices by JAX's collectives and lax.ppermute only.
A program may use at most 64 MiB of HBM per device.

```python
import math
import jax
import jax.numpy as jnp
import numpy as np

CELLS = 524288
VEHICLES = 1024
EVENTS = 1048576


def draw_speed(key, part):
    level_key = jax.random.fold_in(key, 11)
    plant_key = jax.random.fold_in(key, 23)
    levels = jax.random.randint(level_key, (EVENTS,), 0, 65537)
    values = levels.astype(jnp.float32) / 1024.0
    planted = jax.random.randint(plant_key, (EVENTS,), 0, 512)
    values = jnp.where(planted == 0, 64.0, values)
    return values.astype(jnp.float32)


def with_ends(entries, own_key, least, high):
    dims = entries.shape
    index_at = [jax.random.randint(jax.random.fold_in(own_key, axis), (), 0, dims[axis]) for axis in range(len(dims))]
    entries = entries.at[tuple(index_at)].set(least)
    longest = dims.index(max(dims))
    index_at[longest] = (index_at[longest] + 1) % dims[longest]
    return entries.at[tuple(index_at)].set(high)


def ranked_wide(own_key, extent, amount, slope):
    weights = [min(1 << octave, amount + 1 - (1 << octave)) * (1 << 20) // math.isqrt((1 << octave) ** slope) + 1 for octave in range((amount + 1).bit_length()) if 1 << octave <= amount]
    scale = 1 + sum(weights) // (1 << 30)
    listing = np.cumsum(np.array([max(1, weight // scale) for weight in weights]))
    ticket = jax.random.randint(jax.random.fold_in(own_key, 1), extent, 0, int(listing[len(weights) - 1]))
    start = jnp.left_shift(1, jnp.searchsorted(jnp.asarray(listing, jnp.int32), ticket, side="right").astype(jnp.int32))
    rank = start - 1 + jax.random.randint(jax.random.fold_in(own_key, 4), extent, 0, 1 << 30) % jnp.minimum(start, amount + 1 - start)
    return jax.random.permutation(jax.random.fold_in(own_key, 2), amount)[rank].astype(jnp.int32)


def setup_inputs(seed: int = 0) -> dict:
    splits = jax.random.split(jax.random.key(seed), 4)
    cell = with_ends(ranked_wide(splits[0], (EVENTS,), CELLS, 2), jax.random.fold_in(splits[0], 3), 0, CELLS - 1).astype(jnp.int32)
    vehicle = with_ends(jax.random.randint(splits[1], (EVENTS,), 0, VEHICLES), jax.random.fold_in(splits[1], 1), 0, VEHICLES - 1).astype(jnp.int32)
    speed = draw_speed(jax.random.fold_in(splits[3], 71), 0)
    return dict(cell=cell, vehicle=vehicle, speed=speed)


def reference(cell, vehicle, speed):
    top_speed = jnp.full((CELLS,), -1.0, jnp.float32).at[cell].max(speed)
    chosen = jnp.where(speed == top_speed[cell], vehicle, VEHICLES).astype(jnp.int32)
    lowest = jnp.full((CELLS,), VEHICLES, jnp.int32).at[cell].min(chosen)
    top_vehicle = jnp.where(lowest < VEHICLES, lowest, -1).astype(jnp.int32)
    return top_speed, top_vehicle
```

```python
import functools

import jax
import jax.numpy as jnp
from jax import lax
from jax.experimental import pallas as pl
from jax.experimental.pallas import tpu as pltpu
from jax.sharding import PartitionSpec as P

CELLS = 524288
VEHICLES = 1024
STEPS = 1024
AXES = ("gx", "gy")
LANES = 128
ROWS = 8
TILE = ROWS * LANES
BLOCK = LANES * LANES
CUT = 15
LOW = (1 << CUT) - 1


def sub_iota():
    return lax.broadcasted_iota(jnp.int32, (ROWS, LANES), 0)


def lane_iota():
    return lax.broadcasted_iota(jnp.int32, (ROWS, LANES), 1)


def turned(regs):
    out = []
    for first in range(0, len(regs), 16):
        block = jnp.concatenate(regs[first : first + 16], axis=0).T
        out += [block[ROWS * i : ROWS * (i + 1)] for i in range(16)]
    return out


def place(bit, linear):
    if bit >= 14:
        return "v", bit - 10
    if linear:
        return ("l", bit) if bit < 7 else ("s", bit - 7) if bit < 10 else ("v", bit - 10)
    return ("s", bit) if bit < 3 else ("v", bit - 3) if bit < 7 else ("l", bit - 7)


def flip(regs, bit, linear):
    kind, at = place(bit, linear)
    if kind == "v":
        return [~x if g >> at & 1 else x for g, x in enumerate(regs)]
    index = sub_iota() if kind == "s" else lane_iota()
    mask = -((index >> at) & 1)
    return [x ^ mask for x in regs]


def exchange(keys, loads, bit, linear):
    kind, at = place(bit, linear)
    keys, loads = list(keys), list(loads)
    if kind == "v":
        for low in range(len(keys)):
            high = low | 1 << at
            if high == low:
                continue
            a, b, p, q = keys[low], keys[high], loads[low], loads[high]
            swap = a > b
            keys[low], keys[high] = jnp.minimum(a, b), jnp.maximum(a, b)
            loads[low], loads[high] = jnp.where(swap, q, p), jnp.where(swap, p, q)
        return keys, loads
    step = 1 << at
    upper = (sub_iota() >> at & 1) == 1

    def partner(x):
        if 2 * step == ROWS:
            return pltpu.roll(x, step, 0)
        return jnp.where(upper, pltpu.roll(x, step, 0), pltpu.roll(x, ROWS - step, 0))

    for g, (a, p) in enumerate(zip(keys, loads)):
        b, q = partner(a), partner(p)
        new = jnp.where(upper, jnp.maximum(a, b), jnp.minimum(a, b))
        keys[g], loads[g] = new, jnp.where(new == a, p, q)
    return keys, loads


def sort_pairs(keys, loads, first_level, linear):
    bits = (len(keys) * TILE).bit_length() - 1
    for level in range(first_level, bits + 1):
        if level > first_level:
            keys = flip(keys, level - 1, linear)
        if level < bits:
            keys = flip(keys, level, linear)
        for bit in reversed(range(level)):
            if bit < 14 and linear != (bit >= 7):
                keys, loads, linear = turned(keys), turned(loads), not linear
            keys, loads = exchange(keys, loads, bit, linear)
    assert not linear
    return keys, loads


def lane_next(regs, fill):
    rolled = [pltpu.roll(x, LANES - 1, 1) for x in regs]
    rolled.append(jnp.full_like(rolled[0], fill))
    last = lane_iota() == LANES - 1
    return [jnp.where(last, rolled[h + 1], rolled[h]) for h in range(len(regs))]


def pull(regs, bit, linear):
    count = len(regs)
    blocks = count // 16
    kind, at = place(bit, linear)
    zero = jnp.zeros_like(regs[0])
    if kind == "s":
        step = 1 << at
        rolled = [pltpu.roll(x, ROWS - step, 0) for x in regs]
        stay = sub_iota() < ROWS - step
        if linear:
            over = rolled[1:] + [zero]
        else:
            wrap = lane_next([rolled[16 * h] for h in range(blocks)], 0)
            over = [rolled[g + 1] if (g + 1) % 16 else wrap[g // 16] for g in range(count)]
        return [jnp.where(stay, a, b) for a, b in zip(rolled, over)]
    step = 1 << at
    if linear or step >= 16:
        return regs[step:] + [zero] * step
    out = [None] * count
    for v in range(16):
        if v + step < 16:
            for h in range(blocks):
                out[16 * h + v] = regs[16 * h + v + step]
        else:
            wrap = lane_next([regs[16 * h + v + step - 16] for h in range(blocks)], 0)
            for h in range(blocks):
                out[16 * h + v] = wrap[h]
    return out


def push(regs, bit, linear):
    assert len(regs) == 16
    kind, at = place(bit, linear)
    zero = jnp.zeros_like(regs[0])
    first = lane_iota() == 0

    def lane_last(x):
        return jnp.where(first, 0, pltpu.roll(x, 1, 1))

    step = 1 << at
    if kind == "s":
        rolled = [pltpu.roll(x, step, 0) for x in regs]
        over = [zero if linear else lane_last(rolled[15])] + rolled[:15]
        stay = sub_iota() >= step
        return [jnp.where(stay, a, b) for a, b in zip(rolled, over)]
    head = [zero] * step if linear else [lane_last(x) for x in regs[16 - step :]]
    return head + regs[: 16 - step]


def spread_row(x, row):
    return jnp.broadcast_to(x[row : row + 1], (ROWS, LANES))


def down_lanes(row):
    return turned([row] * 16)


def over_rows(regs, op):
    while len(regs) > 1:
        regs = [op(a, b) for a, b in zip(regs[0::2], regs[1::2])]
    x = regs[0]
    for step in (4, 2, 1):
        x = op(x, pltpu.roll(x, step, 0))
    return x


def run_max(cells, keys):
    count = len(cells)
    blocks = count // 16
    sub = sub_iota()
    keys = list(keys)
    for step in (1, 2, 4):
        inside = sub >= step
        for g in range(count):
            same = (pltpu.roll(cells[g], step, 0) == cells[g]) & inside
            keys[g] = jnp.where(same, jnp.maximum(keys[g], pltpu.roll(keys[g], step, 0)), keys[g])
    for h in range(blocks):
        for v in range(1, 16):
            g = 16 * h + v
            cell, key = spread_row(cells[g - 1], 7), spread_row(keys[g - 1], 7)
            keys[g] = jnp.where(cells[g] == cell, jnp.maximum(keys[g], key), keys[g])
    last_cell = [spread_row(cells[16 * h + 15], 7) for h in range(blocks)]
    last_key = [spread_row(keys[16 * h + 15], 7) for h in range(blocks)]
    rolled = [jnp.full((ROWS, LANES), -9, jnp.int32)] + [pltpu.roll(x, 1, 1) for x in last_cell]
    lane = lane_iota()
    before = [jnp.where(lane == 0, rolled[h], rolled[h + 1]) for h in range(blocks)]
    cell_col = [down_lanes(x) for x in last_cell]
    key_col = [down_lanes(x) for x in last_key]
    for h in range(blocks):
        terms = []
        for source in range(h + 1):
            for v in range(16):
                match = cell_col[source][v] == before[h]
                if source == h:
                    match = match & (sub + ROWS * v < lane)
                terms.append((match, key_col[source][v]))
        terms = [jnp.where(match, key, -1) for match, key in terms]
        while len(terms) % 16 or len(terms) & (len(terms) - 1):
            terms.append(terms[0])
        best = over_rows(terms, jnp.maximum)
        for g in range(16 * h, 16 * h + 16):
            keys[g] = jnp.where(cells[g] == before[h], jnp.maximum(keys[g], best), keys[g])
    return keys


def run_ends(cells):
    count = len(cells)
    rolled = [pltpu.roll(x, ROWS - 1, 0) for x in cells]
    wrap = lane_next([rolled[16 * h] for h in range(count // 16)], -9)
    over = [rolled[g + 1] if (g + 1) % 16 else wrap[g // 16] for g in range(count)]
    bottom = sub_iota() == ROWS - 1
    return [c != jnp.where(bottom, b, a) for c, a, b in zip(cells, rolled, over)]


def ranks(flags):
    count = len(flags)
    blocks = count // 16
    sub, lane = sub_iota(), lane_iota()
    out, total = [], jnp.zeros((ROWS, LANES), jnp.int32)
    for h in range(blocks):
        sums, run = [], jnp.zeros((ROWS, LANES), jnp.int32)
        for v in range(16):
            flag = flags[16 * h + v]
            x = flag
            for step in (1, 2, 4):
                x = x + jnp.where(sub >= step, pltpu.roll(x, step, 0), 0)
            sums.append(x - flag + run)
            run = run + spread_row(x, 7)
        col = down_lanes(run)
        start = [jnp.where(sub + ROWS * v < lane, col[v], 0) for v in range(16)]
        start = over_rows(start, jnp.add) + total
        total = total + over_rows(col, jnp.add)
        out += [x + start for x in sums]
    return out, total


def positions(count, linear):
    sub, lane = sub_iota(), lane_iota()
    if linear:
        return [TILE * g + LANES * sub + lane for g in range(count)]
    return [BLOCK * (g // 16) + LANES * lane + ROWS * (g % 16) + sub for g in range(count)]


def travel(move, load, bit, linear, shift, empty):
    probe = 1 << (CUT + bit)
    new_move, new_load = shift(move, bit, linear), shift(load, bit, linear)
    for g in range(len(move)):
        arrives = (new_move[g] & probe) != 0
        leaves = (move[g] & probe) != 0
        stay = load[g] if empty is None else jnp.where(leaves, empty, load[g])
        new_move[g] = jnp.where(arrives, new_move[g], jnp.where(leaves, 0, move[g]))
        new_load[g] = jnp.where(arrives, new_load[g], stay)
    return new_move, new_load


def compact(cells, keys, wanted):
    count = len(cells)
    rank, total = ranks([jnp.where(w, 1, 0) for w in wanted])
    at = positions(count, False)
    move = [
        jnp.where(w, (i - r) << CUT | c, 0) for w, i, r, c in zip(wanted, at, rank, cells)
    ]
    for bit in range((count * TILE).bit_length() - 1):
        if bit == 7:
            move, keys = turned(move), turned(keys)
        move, keys = travel(move, keys, bit, bit >= 7, pull, None)
    return [x & LOW for x in move], keys, total


def split_kernel(own, slots, chunk, round_ref, odd_ref, cell_ref, vehicle_ref, speed_ref, out_ref, low_ref, high_ref):
    n = CELLS // own
    count = cell_ref.shape[0] // ROWS
    odd = odd_ref[0]
    cells, keys = [], []
    for g in range(count):
        at = pl.ds(ROWS * g, ROWS)
        cell = cell_ref[at, :]
        cells.append(jnp.where(odd == 1, CELLS - 1 - cell, cell))
        level = (speed_ref[at, :] * float(STEPS)).astype(jnp.int32)
        keys.append(level * VEHICLES + (VEHICLES - 1 - vehicle_ref[at, :]))
    cells, keys = sort_pairs(cells, keys, 1, False)
    keys = run_max(cells, keys)
    ends = run_ends(cells)
    shift = own.bit_length() - 1
    owner = [jnp.where(w, c >> shift, -1) for w, c in zip(ends, cells)]
    high = [k | (c >> CUT) << 27 for k, c in zip(keys, cells)]
    low, high, _ = compact([c & LOW for c in cells], high, ends)
    for g in range(count):
        at = pl.ds(ROWS * g, ROWS)
        low_ref[at, :] = low[g]
        high_ref[at, :] = high[g]
    low_ref[pl.ds(ROWS * count, ROWS), :] = jnp.zeros((ROWS, LANES), jnp.int32)
    high_ref[pl.ds(ROWS * count, ROWS), :] = jnp.zeros((ROWS, LANES), jnp.int32)
    sizes = [jnp.sum(sum(jnp.where(w == o, 1, 0) for w in owner)) for o in range(n)]
    most = functools.reduce(jnp.maximum, sizes)
    sub, lane = sub_iota(), lane_iota()
    skip = round_ref[0] * (slots * LANES)
    base = jnp.int32(0)
    for o in range(n):
        start = base + skip
        valid = sub * LANES + lane < sizes[o] - skip
        start = jnp.minimum(start, count * TILE)
        base = base + sizes[o]
        row, off = start >> 7, start & 127

        def window(ref):
            x = pltpu.roll(ref[pl.ds(row, ROWS), :], (LANES - off) & 127, 1)
            return jnp.where(lane < LANES - off, x, pltpu.roll(x, ROWS - 1, 0))

        low_w, high_w = window(low_ref), window(high_ref)
        cell = jnp.where(valid, low_w & (own - 1), own).astype(jnp.float32)
        key = jnp.where(valid, high_w & ((1 << 27) - 1), 0)
        speed = (key >> 10).astype(jnp.float32) * (1.0 / STEPS)
        ident = (VEHICLES - 1 - (key & (VEHICLES - 1))).astype(jnp.float32)
        target = pl.multiple_of(jnp.where(odd == 1, n - 1 - o, o) * chunk, chunk)
        for w, x in enumerate((cell, speed, ident)):
            out_ref[pl.ds(target + w * slots, slots), :] = x[:slots]
        tail = chunk - 3 * slots
        fill = jnp.full((tail, LANES), most.astype(jnp.float32))
        out_ref[pl.ds(target + 3 * slots, tail), :] = fill


def join_kernel(own, n, slots, chunk, in_ref, speed_ref, ident_ref, most_ref):
    sub = sub_iota()
    per = ROWS // run_rows(slots)
    cells, keys = [], []
    most = jnp.zeros((1, LANES), jnp.float32)
    for g in range(n // per):
        if per == 1:
            part = [in_ref[pl.ds(chunk * g + w * slots, slots), :] for w in range(3)]
            pad = jnp.zeros((ROWS - slots, LANES), jnp.float32)
            part = [jnp.concatenate([x, pad], axis=0) for x in part]
            live = sub < slots
            source = g & 1
        else:
            part = [in_ref[pl.ds(chunk * per * g + w, ROWS, stride=chunk), :] for w in range(3)]
            live = sub >= 0
            source = sub & 1
        for k in range(per):
            most = jnp.maximum(most, in_ref[pl.ds(chunk * (per * g + k + 1) - 1, 1), :])
        cell = jnp.where(live, part[0].astype(jnp.int32), own)
        if per == 1:
            cell = own - 1 - cell if source else cell
        else:
            cell = jnp.where(source == 1, own - 1 - cell, cell)
        level = (part[1] * float(STEPS)).astype(jnp.int32)
        cells.append(cell)
        keys.append(level * VEHICLES + (VEHICLES - 1 - part[2].astype(jnp.int32)))
    most_ref[...] = most
    first = (run_rows(slots) * LANES).bit_length()
    cells, keys = sort_pairs(cells, keys, first, True)
    keys = run_max(cells, keys)
    ends = [w & (c >= 0) & (c < own) for w, c in zip(run_ends(cells), cells)]
    cells, keys, total = compact(cells, keys, ends)
    keep = max(own // TILE, 1)
    at = positions(16, True)
    move = [jnp.where(i < total, (c - i) << CUT, 0) for i, c in zip(at, cells)]
    keys = [jnp.where(i < total, k, -1) for i, k in zip(at, keys)]
    linear = True
    for bit in reversed(range(own.bit_length() - 1)):
        if bit == 6:
            move, keys, linear = turned(move), turned(keys), False
        move, keys = travel(move, keys, bit, linear, push, -1)
    keys = turned(keys)
    for g in range(keep):
        key = keys[g]
        at = pl.ds(ROWS * g, ROWS)
        speed = (key >> 10).astype(jnp.float32) * (1.0 / STEPS)
        speed_ref[at, :] = jnp.where(key >= 0, speed, -1.0)
        ident_ref[at, :] = jnp.where(key >= 0, VEHICLES - 1 - (key & (VEHICLES - 1)), -1)


def run_rows(slots):
    return 1 << (slots - 1).bit_length()


def per_device(cell, vehicle, speed):
    n = lax.axis_size(AXES)
    own = CELLS // n
    events = cell.shape[0]
    slots = max(1, (5 * events // n) // (8 * LANES))
    chunk = -(-(3 * slots + 1) // ROWS) * ROWS
    rows = events // LANES
    smem = pl.BlockSpec(memory_space=pltpu.SMEM)
    vmem = pl.BlockSpec(memory_space=pltpu.VMEM)
    table = (own // LANES, LANES)
    odd = (lax.axis_index(AXES) & 1).reshape(1)
    inputs = [x.reshape(rows, LANES) for x in (cell, vehicle, speed)]

    split = pl.pallas_call(
        functools.partial(split_kernel, own, slots, chunk),
        out_shape=jax.ShapeDtypeStruct((n * chunk, LANES), jnp.float32),
        in_specs=[smem, smem, vmem, vmem, vmem],
        out_specs=vmem,
        scratch_shapes=[pltpu.VMEM((rows + ROWS, LANES), jnp.int32)] * 2,
        name="split",
    )
    join = pl.pallas_call(
        functools.partial(join_kernel, own, n, slots, chunk),
        out_shape=(
            jax.ShapeDtypeStruct(table, jnp.float32),
            jax.ShapeDtypeStruct(table, jnp.int32),
            jax.ShapeDtypeStruct((1, LANES), jnp.float32),
        ),
        in_specs=[vmem],
        out_specs=(vmem, vmem, vmem),
        name="join",
    )

    def one_round(index):
        sent = split(index.reshape(1), odd, *inputs)
        got = lax.all_to_all(sent.reshape(n, chunk, LANES), AXES, 0, 0, tiled=True)
        return join(got.reshape(n * chunk, LANES))

    best, ident, most = one_round(jnp.int32(0))
    rounds = -(-most[0, 0].astype(jnp.int32) // (slots * LANES))

    def again(state):
        index, best, ident = state
        more, other, _ = one_round(index)
        ident = jnp.where(
            more > best, other, jnp.where(more < best, ident, jnp.minimum(ident, other))
        )
        return index + 1, jnp.maximum(best, more), ident

    _, best, ident = lax.while_loop(
        lambda state: state[0] < rounds, again, (jnp.int32(1), best, ident)
    )
    return best.reshape(own), ident.reshape(own)


def solution(mesh):
    placed = P(AXES)
    return jax.shard_map(
        per_device,
        mesh=mesh,
        in_specs=(placed, placed, placed),
        out_specs=(placed, placed),
        check_vma=False,
    )
```

```python
import functools

import jax
import jax.numpy as jnp
from jax import lax
from jax.experimental import pallas as pl
from jax.experimental.pallas import tpu as pltpu
from jax.sharding import PartitionSpec as P

CELLS = 524288
VEHICLES = 1024
STEPS = 1024
AXES = ("gx", "gy")
LANES = 128
ROWS = 8
TILE = ROWS * LANES
BLOCK = LANES * LANES
CUT = 15
LOW = (1 << CUT) - 1
PITCH = ROWS + 1


def sub_iota():
    return lax.broadcasted_iota(jnp.int32, (ROWS, LANES), 0)


def lane_iota():
    return lax.broadcasted_iota(jnp.int32, (ROWS, LANES), 1)


def turned(regs):
    out = []
    for first in range(0, len(regs), 16):
        block = jnp.concatenate(regs[first : first + 16], axis=0).T
        out += [block[ROWS * i : ROWS * (i + 1)] for i in range(16)]
    return out


def place(bit, linear):
    if bit >= 14:
        return "v", bit - 10
    if linear:
        return ("l", bit) if bit < 7 else ("s", bit - 7) if bit < 10 else ("v", bit - 10)
    return ("s", bit) if bit < 3 else ("v", bit - 3) if bit < 7 else ("l", bit - 7)


def flip(regs, spot):
    kind, at = spot
    if kind == "v":
        return [~x if g >> at & 1 else x for g, x in enumerate(regs)]
    index = sub_iota() if kind == "s" else lane_iota()
    mask = -((index >> at) & 1)
    return [x ^ mask for x in regs]


def swapped(regs, ref):
    for g, x in enumerate(regs):
        ref[pl.ds(PITCH * g, ROWS), :] = x
    return [
        ref[pl.ds(PITCH * (g & ~7) + (g & 7), ROWS, stride=PITCH), :] for g in range(len(regs))
    ]


def sort_levels(keys, loads, spots, levels, key_ref, load_ref):
    bits = len(spots)

    def moved(pairs, change):
        names = dict(pairs) | {b: a for a, b in pairs}
        spots[:] = [names.get(spot, spot) for spot in spots]
        keys[:], loads[:] = change(keys, key_ref), change(loads, load_ref)

    def turn():
        pairs = [(("s", b), ("l", b)) for b in range(3)]
        pairs += [(("v", b), ("l", b + 3)) for b in range(4)]
        moved(pairs, lambda regs, ref: turned(regs))

    def swap():
        moved([(("s", b), ("v", b)) for b in range(3)], swapped)

    for level in levels:
        if level > levels[0]:
            keys[:] = flip(keys, spots[level - 1])
        if level < bits:
            keys[:] = flip(keys, spots[level])
        for bit in reversed(range(level)):
            if spots[bit][0] == "l":
                if level == bits and bit < 7 and spots[7][0] == "v":
                    swap()
                turn()
            if spots[bit][0] == "s":
                swap()
            at = spots[bit][1]
            for low in range(len(keys)):
                high = low | 1 << at
                if high == low:
                    continue
                a, b, p, q = keys[low], keys[high], loads[low], loads[high]
                larger = a > b
                keys[low], keys[high] = jnp.minimum(a, b), jnp.maximum(a, b)
                loads[low], loads[high] = jnp.where(larger, q, p), jnp.where(larger, p, q)
    if levels[-1] < bits:
        keys[:] = flip(keys, spots[levels[-1]])
    elif spots[0][0] == "v":
        swap()


def lane_next(regs, fill):
    rolled = [pltpu.roll(x, LANES - 1, 1) for x in regs]
    rolled.append(jnp.full_like(rolled[0], fill))
    last = lane_iota() == LANES - 1
    return [jnp.where(last, rolled[h + 1], rolled[h]) for h in range(len(regs))]


def pull(regs, bit, linear):
    count = len(regs)
    blocks = count // 16
    kind, at = place(bit, linear)
    zero = jnp.zeros_like(regs[0])
    if kind == "s":
        step = 1 << at
        rolled = [pltpu.roll(x, ROWS - step, 0) for x in regs]
        stay = sub_iota() < ROWS - step
        if linear:
            over = rolled[1:] + [zero]
        else:
            wrap = lane_next([rolled[16 * h] for h in range(blocks)], 0)
            over = [rolled[g + 1] if (g + 1) % 16 else wrap[g // 16] for g in range(count)]
        return [jnp.where(stay, a, b) for a, b in zip(rolled, over)]
    step = 1 << at
    if linear or step >= 16:
        return regs[step:] + [zero] * step
    out = [None] * count
    for v in range(16):
        if v + step < 16:
            for h in range(blocks):
                out[16 * h + v] = regs[16 * h + v + step]
        else:
            wrap = lane_next([regs[16 * h + v + step - 16] for h in range(blocks)], 0)
            for h in range(blocks):
                out[16 * h + v] = wrap[h]
    return out


def push(regs, bit, linear):
    assert len(regs) == 16
    kind, at = place(bit, linear)
    zero = jnp.zeros_like(regs[0])
    first = lane_iota() == 0

    def lane_last(x):
        return jnp.where(first, 0, pltpu.roll(x, 1, 1))

    step = 1 << at
    if kind == "s":
        rolled = [pltpu.roll(x, step, 0) for x in regs]
        over = [zero if linear else lane_last(rolled[15])] + rolled[:15]
        stay = sub_iota() >= step
        return [jnp.where(stay, a, b) for a, b in zip(rolled, over)]
    head = [zero] * step if linear else [lane_last(x) for x in regs[16 - step :]]
    return head + regs[: 16 - step]


def spread_row(x, row):
    return jnp.broadcast_to(x[row : row + 1], (ROWS, LANES))


def down_lanes(row):
    return turned([row] * 16)


def over_rows(regs, op):
    while len(regs) > 1:
        regs = [op(a, b) for a, b in zip(regs[0::2], regs[1::2])]
    x = regs[0]
    for step in (4, 2, 1):
        x = op(x, pltpu.roll(x, step, 0))
    return x


def run_max(cells, keys):
    count = len(cells)
    blocks = count // 16
    sub = sub_iota()
    keys = list(keys)
    for step in (1, 2, 4):
        inside = sub >= step
        for g in range(count):
            same = (pltpu.roll(cells[g], step, 0) == cells[g]) & inside
            keys[g] = jnp.where(same, jnp.maximum(keys[g], pltpu.roll(keys[g], step, 0)), keys[g])
    for h in range(blocks):
        for v in range(1, 16):
            g = 16 * h + v
            cell, key = spread_row(cells[g - 1], 7), spread_row(keys[g - 1], 7)
            keys[g] = jnp.where(cells[g] == cell, jnp.maximum(keys[g], key), keys[g])
    last_cell = [spread_row(cells[16 * h + 15], 7) for h in range(blocks)]
    last_key = [spread_row(keys[16 * h + 15], 7) for h in range(blocks)]
    rolled = [jnp.full((ROWS, LANES), -9, jnp.int32)] + [pltpu.roll(x, 1, 1) for x in last_cell]
    lane = lane_iota()
    before = [jnp.where(lane == 0, rolled[h], rolled[h + 1]) for h in range(blocks)]
    cell_col = [down_lanes(x) for x in last_cell]
    key_col = [down_lanes(x) for x in last_key]
    for h in range(blocks):
        terms = []
        for source in range(h + 1):
            for v in range(16):
                match = cell_col[source][v] == before[h]
                if source == h:
                    match = match & (sub + ROWS * v < lane)
                terms.append((match, key_col[source][v]))
        terms = [jnp.where(match, key, -1) for match, key in terms]
        while len(terms) % 16 or len(terms) & (len(terms) - 1):
            terms.append(terms[0])
        best = over_rows(terms, jnp.maximum)
        for g in range(16 * h, 16 * h + 16):
            keys[g] = jnp.where(cells[g] == before[h], jnp.maximum(keys[g], best), keys[g])
    return keys


def run_ends(cells):
    count = len(cells)
    rolled = [pltpu.roll(x, ROWS - 1, 0) for x in cells]
    wrap = lane_next([rolled[16 * h] for h in range(count // 16)], -9)
    over = [rolled[g + 1] if (g + 1) % 16 else wrap[g // 16] for g in range(count)]
    bottom = sub_iota() == ROWS - 1
    return [c != jnp.where(bottom, b, a) for c, a, b in zip(cells, rolled, over)]


def ranks(flags):
    count = len(flags)
    blocks = count // 16
    sub, lane = sub_iota(), lane_iota()
    out, total = [], jnp.zeros((ROWS, LANES), jnp.int32)
    for h in range(blocks):
        sums, run = [], jnp.zeros((ROWS, LANES), jnp.int32)
        for v in range(16):
            flag = flags[16 * h + v]
            x = flag
            for step in (1, 2, 4):
                x = x + jnp.where(sub >= step, pltpu.roll(x, step, 0), 0)
            sums.append(x - flag + run)
            run = run + spread_row(x, 7)
        col = down_lanes(run)
        start = [jnp.where(sub + ROWS * v < lane, col[v], 0) for v in range(16)]
        start = over_rows(start, jnp.add) + total
        total = total + over_rows(col, jnp.add)
        out += [x + start for x in sums]
    return out, total


def positions(count, linear):
    sub, lane = sub_iota(), lane_iota()
    if linear:
        return [TILE * g + LANES * sub + lane for g in range(count)]
    return [BLOCK * (g // 16) + LANES * lane + ROWS * (g % 16) + sub for g in range(count)]


def travel(move, load, bit, linear, shift, empty):
    probe = 1 << (CUT + bit)
    new_move, new_load = shift(move, bit, linear), shift(load, bit, linear)
    for g in range(len(move)):
        arrives = (new_move[g] & probe) != 0
        old_move, old_load = move[g], load[g]
        if empty is not None:
            leaves = (old_move & probe) != 0
            old_move, old_load = jnp.where(leaves, 0, old_move), jnp.where(leaves, empty, old_load)
        new_move[g] = jnp.where(arrives, new_move[g], old_move)
        new_load[g] = jnp.where(arrives, new_load[g], old_load)
    return new_move, new_load


def compact(cells, keys, wanted):
    count = len(cells)
    rank, total = ranks([jnp.where(w, 1, 0) for w in wanted])
    at = positions(count, False)
    move = [
        jnp.where(w, (i - r) << CUT | c, 0) for w, i, r, c in zip(wanted, at, rank, cells)
    ]
    for bit in range((count * TILE).bit_length() - 1):
        if bit == 7:
            move, keys = turned(move), turned(keys)
        move, keys = travel(move, keys, bit, bit >= 7, pull, None)
    return [x & LOW for x in move], keys, total


def owner_sizes(flags, cells, n, shift):
    sums = [jnp.zeros((ROWS, LANES), jnp.int32)] * (n // 4)
    for w, c in zip(flags, cells):
        group = jnp.where(w, c >> (shift + 2), -1)
        unit = jnp.left_shift(1, (c >> (shift - 3)) & 24)
        sums = [x + jnp.where(group == k, unit, 0) for k, x in enumerate(sums)]
    sizes = []
    for x in sums:
        pairs = []
        for part in (x & 0xFF00FF, (x >> 8) & 0xFF00FF):
            for step in (4, 2, 1):
                part = part + pltpu.roll(part, step, 0)
            pairs.append(part)
        for half in (0, 16):
            for part in pairs:
                row = (part >> half) & 0xFFFF
                sizes.append(jnp.sum(jnp.where(sub_iota() == 0, row, 0)))
    return sizes


def split_kernel(own, slots, chunk, round_ref, odd_ref, cell_in, vehicle_in, speed_in, out_hbm, cell_ref, vehicle_ref, speed_ref, out_ref, low_ref, high_ref, cell_pad, key_pad, in_sem, out_sem):
    n = CELLS // own
    count = cell_ref.shape[0] // ROWS
    bits = (count * TILE).bit_length() - 1
    odd = odd_ref[0]
    arrays = ((cell_in, cell_ref), (vehicle_in, vehicle_ref), (speed_in, speed_ref))
    copies = []
    for h in range(count // 16):
        part = pl.ds(LANES * h, LANES)
        copies.append(
            [
                pltpu.make_async_copy(x.at[part, :], y.at[part, :], in_sem.at[h, k])
                for k, (x, y) in enumerate(arrays)
            ]
        )
        for copy in copies[h]:
            copy.start()
    cells, keys = [], []
    for h in range(count // 16):
        for copy in copies[h]:
            copy.wait()
        some_cells, some_keys = [], []
        for g in range(16 * h, 16 * h + 16):
            at = pl.ds(ROWS * g, ROWS)
            cell = cell_ref[at, :]
            some_cells.append(jnp.where(odd == 1, CELLS - 1 - cell, cell))
            level = (speed_ref[at, :] * float(STEPS)).astype(jnp.int32)
            some_keys.append(level * VEHICLES + (VEHICLES - 1 - vehicle_ref[at, :]))
        spots = [place(bit, False) for bit in range(bits)]
        pad = pl.ds(16 * PITCH * h, 16 * PITCH)
        sort_levels(
            some_cells, some_keys, spots, range(1, 8), cell_pad.at[pad, :], key_pad.at[pad, :]
        )
        cells += some_cells
        keys += some_keys
    sort_levels(cells, keys, spots, range(8, bits + 1), cell_pad, key_pad)
    keys = run_max(cells, keys)
    ends = run_ends(cells)
    shift = own.bit_length() - 1
    sizes = owner_sizes(ends, cells, n, shift)
    high = [k | (c >> CUT) << 27 for k, c in zip(keys, cells)]
    low, high, _ = compact([c & LOW for c in cells], high, ends)
    for g in range(count):
        at = pl.ds(ROWS * g, ROWS)
        low_ref[at, :] = low[g]
        high_ref[at, :] = high[g]
    low_ref[pl.ds(ROWS * count, ROWS), :] = jnp.zeros((ROWS, LANES), jnp.int32)
    high_ref[pl.ds(ROWS * count, ROWS), :] = jnp.zeros((ROWS, LANES), jnp.int32)
    most = functools.reduce(jnp.maximum, sizes)
    sub, lane = sub_iota(), lane_iota()
    skip = round_ref[0] * (slots * LANES)
    base = jnp.int32(0)
    group = n // 4
    writes = []
    for k in range(4):
        part = pl.ds(jnp.where(odd == 1, 3 - k, k) * (group * chunk), group * chunk)
        writes.append(
            pltpu.make_async_copy(out_ref.at[part, :], out_hbm.at[part, :], out_sem.at[k])
        )
    for o in range(n):
        if o % group == 0 and o > group:
            writes[o // group - 2].start()
        start = base + skip
        valid = sub * LANES + lane < sizes[o] - skip
        start = jnp.minimum(start, count * TILE)
        base = base + sizes[o]
        row, off = start >> 7, start & 127

        def window(ref):
            x = pltpu.roll(ref[pl.ds(row, ROWS), :], (LANES - off) & 127, 1)
            return jnp.where(lane < LANES - off, x, pltpu.roll(x, ROWS - 1, 0))

        low_w, high_w = window(low_ref), window(high_ref)
        cell = jnp.where(valid, low_w & (own - 1), own).astype(jnp.float32)
        level = (high_w & ((1 << 27) - 1)) >> 10
        speed = level.astype(jnp.float32) * (1.0 / STEPS)
        ident = (~high_w & (VEHICLES - 1)).astype(jnp.float32)
        target = pl.multiple_of(jnp.where(odd == 1, n - 1 - o, o) * chunk, chunk)
        for w, x in enumerate((cell, speed, ident)):
            out_ref[pl.ds(target + w * slots, slots), :] = x[:slots]
        tail = chunk - 3 * slots
        fill = jnp.full((tail, LANES), most.astype(jnp.float32))
        out_ref[pl.ds(target + 3 * slots, tail), :] = fill
    for k in (2, 3):
        writes[k].start()
    for write in writes:
        write.wait()


def join_kernel(own, n, slots, chunk, in_ref, speed_ref, ident_ref, rounds_ref, cell_pad, key_pad):
    sub = sub_iota()
    per = ROWS // run_rows(slots)
    cells, keys = [], []
    most = jnp.zeros((ROWS, LANES), jnp.float32)
    for g in range(n // per):
        if per == 1:
            part = [in_ref[pl.ds(chunk * g + w * slots, slots), :] for w in range(3)]
            pad = jnp.zeros((ROWS - slots, LANES), jnp.float32)
            part = [jnp.concatenate([x, pad], axis=0) for x in part]
            live = sub < slots
            source = g & 1
        else:
            part = [in_ref[pl.ds(chunk * per * g + w, ROWS, stride=chunk), :] for w in range(3)]
            live = sub >= 0
            source = sub & 1
        for k in range(per):
            most = jnp.maximum(most, in_ref[pl.ds(chunk * (per * g + k + 1) - ROWS, ROWS), :])
        cell = jnp.where(live, part[0].astype(jnp.int32), own)
        if per == 1:
            cell = own - 1 - cell if source else cell
        else:
            cell = jnp.where(source == 1, own - 1 - cell, cell)
        level = (part[1] * float(STEPS)).astype(jnp.int32)
        cells.append(cell)
        keys.append(level * VEHICLES + (VEHICLES - 1 - part[2].astype(jnp.int32)))
    most = jnp.max(jnp.where(sub == ROWS - 1, most, 0.0)).astype(jnp.int32)
    rounds_ref[0] = lax.div(most + (slots * LANES - 1), jnp.int32(slots * LANES))
    first = (run_rows(slots) * LANES).bit_length()
    bits = (len(cells) * TILE).bit_length() - 1
    spots = [place(bit, True) for bit in range(bits)]
    sort_levels(cells, keys, spots, range(first, bits + 1), cell_pad, key_pad)
    keys = run_max(cells, keys)
    ends = [w & (c >= 0) & (c < own) for w, c in zip(run_ends(cells), cells)]
    cells, keys, total = compact(cells, keys, ends)
    keep = max(own // TILE, 1)
    at = positions(16, True)
    move = [jnp.where(i < total, (c - i) << CUT, 0) for i, c in zip(at, cells)]
    keys = [jnp.where(i < total, k, -1) for i, k in zip(at, keys)]
    linear = True
    for bit in reversed(range(own.bit_length() - 1)):
        if bit == 6:
            move, keys, linear = turned(move), turned(keys), False
        move, keys = travel(move, keys, bit, linear, push, -1)
    keys = turned(keys)
    for g in range(keep):
        key = keys[g]
        at = pl.ds(ROWS * g, ROWS)
        speed = (key >> 10).astype(jnp.float32) * (1.0 / STEPS)
        speed_ref[at, :] = jnp.where(key >= 0, speed, -1.0)
        ident_ref[at, :] = jnp.where(key >= 0, VEHICLES - 1 - (key & (VEHICLES - 1)), -1)


def run_rows(slots):
    return 1 << (slots - 1).bit_length()


def pads(rows):
    return [pltpu.VMEM((rows // ROWS * PITCH, LANES), jnp.int32)] * 2


def per_device(cell, vehicle, speed):
    n = lax.axis_size(AXES)
    own = CELLS // n
    events = cell.shape[0]
    slots = max(1, (5 * events // n) // (8 * LANES))
    chunk = -(-(3 * slots + 1) // ROWS) * ROWS
    rows = events // LANES
    smem = pl.BlockSpec(memory_space=pltpu.SMEM)
    vmem = pl.BlockSpec(memory_space=pltpu.VMEM)
    hbm = pl.BlockSpec(memory_space=pl.ANY)
    params = pltpu.CompilerParams(vmem_limit_bytes=16 << 20)
    table = (own // LANES, LANES)
    odd = (lax.axis_index(AXES) & 1).reshape(1)
    inputs = [x.reshape(rows, LANES) for x in (cell, vehicle, speed)]

    split = pl.pallas_call(
        functools.partial(split_kernel, own, slots, chunk),
        out_shape=jax.ShapeDtypeStruct((n * chunk, LANES), jnp.float32),
        in_specs=[smem, smem, hbm, hbm, hbm],
        out_specs=hbm,
        scratch_shapes=[
            pltpu.VMEM((rows, LANES), jnp.int32),
            pltpu.VMEM((rows, LANES), jnp.int32),
            pltpu.VMEM((rows, LANES), jnp.float32),
            pltpu.VMEM((n * chunk, LANES), jnp.float32),
            pltpu.VMEM((rows + ROWS, LANES), jnp.int32),
            pltpu.VMEM((rows + ROWS, LANES), jnp.int32),
        ]
        + pads(rows)
        + [pltpu.SemaphoreType.DMA((rows // LANES, 3)), pltpu.SemaphoreType.DMA((4,))],
        compiler_params=params,
        name="split",
    )
    join = pl.pallas_call(
        functools.partial(join_kernel, own, n, slots, chunk),
        out_shape=(
            jax.ShapeDtypeStruct(table, jnp.float32),
            jax.ShapeDtypeStruct(table, jnp.int32),
            jax.ShapeDtypeStruct((1,), jnp.int32),
        ),
        in_specs=[vmem],
        out_specs=(vmem, vmem, smem),
        scratch_shapes=pads(n * run_rows(slots)),
        compiler_params=params,
        name="join",
    )

    def one_round(index):
        sent = split(index.reshape(1), odd, *inputs)
        got = lax.all_to_all(sent.reshape(n, chunk, LANES), AXES, 0, 0, tiled=True)
        return join(got.reshape(n * chunk, LANES))

    best, ident, rounds = one_round(jnp.int32(0))

    def again(state):
        index, best, ident = state
        more, other, _ = one_round(index)
        ident = jnp.where(
            more > best, other, jnp.where(more < best, ident, jnp.minimum(ident, other))
        )
        return index + 1, jnp.maximum(best, more), ident

    _, best, ident = lax.while_loop(
        lambda state: state[0] < rounds[0], again, (jnp.int32(1), best, ident)
    )
    return best.reshape(own), ident.reshape(own)


def solution(mesh):
    placed = P(AXES)
    return jax.shard_map(
        per_device,
        mesh=mesh,
        in_specs=(placed, placed, placed),
        out_specs=(placed, placed),
        check_vma=False,
    )
```

```python
import functools

import jax
import jax.numpy as jnp
from jax import lax
from jax.experimental import pallas as pl
from jax.experimental.pallas import tpu as pltpu
from jax.sharding import PartitionSpec as P

CELLS = 524288
VEHICLES = 1024
STEPS = 1024
AXES = ("gx", "gy")
LANES = 128
ROWS = 8
TILE = ROWS * LANES
BLOCK = LANES * LANES
CUT = 15
LOW = (1 << CUT) - 1
PITCH = ROWS + 1


def sub_iota():
    return lax.broadcasted_iota(jnp.int32, (ROWS, LANES), 0)


def lane_iota():
    return lax.broadcasted_iota(jnp.int32, (ROWS, LANES), 1)


def turned(regs):
    out = []
    for first in range(0, len(regs), 16):
        block = jnp.concatenate(regs[first : first + 16], axis=0).T
        out += [block[ROWS * i : ROWS * (i + 1)] for i in range(16)]
    return out


def place(bit, linear):
    if bit >= 14:
        return "v", bit - 10
    if linear:
        return ("l", bit) if bit < 7 else ("s", bit - 7) if bit < 10 else ("v", bit - 10)
    return ("s", bit) if bit < 3 else ("v", bit - 3) if bit < 7 else ("l", bit - 7)


def swapped(regs, ref):
    for g, x in enumerate(regs):
        ref[pl.ds(PITCH * g, ROWS), :] = x
    return [
        ref[pl.ds(PITCH * (g & ~7) + (g & 7), ROWS, stride=PITCH), :] for g in range(len(regs))
    ]


def exchange(keys, loads, low, high, more_keys=None, more_loads=None):
    more_keys = keys if more_keys is None else more_keys
    more_loads = loads if more_loads is None else more_loads
    a, b, p, q = keys[low], more_keys[high], loads[low], more_loads[high]
    larger = a > b
    keys[low], more_keys[high] = jnp.minimum(a, b), jnp.maximum(a, b)
    loads[low], more_loads[high] = jnp.where(larger, q, p), jnp.where(larger, p, q)


class Block:
    def __init__(self, load, index, linear, key_ref, load_ref):
        self.load, self.index = load, index
        self.spots = [place(bit, linear) for bit in range(14)]
        at = pl.ds(16 * PITCH * index, 16 * PITCH)
        self.refs = key_ref.at[at, :], load_ref.at[at, :]
        self.faced = None

    def moved(self, pairs, change):
        names = dict(pairs) | {b: a for a, b in pairs}
        self.spots = [names.get(spot, spot) for spot in self.spots]
        self.keys = change(self.keys, self.refs[0])
        self.loads = change(self.loads, self.refs[1])

    def turn(self):
        pairs = [(("s", b), ("l", b)) for b in range(3)]
        pairs += [(("v", b), ("l", b + 3)) for b in range(4)]
        self.moved(pairs, lambda regs, ref: turned(regs))

    def swap(self):
        self.moved([(("s", b), ("v", b)) for b in range(3)], swapped)

    def face(self, bit):
        odd, mask = [0] * 16, None
        for each in {self.faced, bit} - {None}:
            kind, at = self.spots[each] if each < 14 else ("h", each - 14)
            if kind == "h":
                odd = [x ^ (self.index >> at & 1) for x in odd]
            elif kind == "v":
                odd = [x ^ (g >> at & 1) for g, x in enumerate(odd)]
            else:
                index = sub_iota() if kind == "s" else lane_iota()
                one = -((index >> at) & 1)
                mask = one if mask is None else mask ^ one
        if mask is None:
            self.keys = [~x if o else x for x, o in zip(self.keys, odd)]
        else:
            masks = mask, ~mask
            self.keys = [x ^ masks[o] for x, o in zip(self.keys, odd)]
        self.faced = bit

    def levels(self, levels, bits):
        if self.load is not None:
            self.keys, self.loads = self.load()
            self.load = None
        for level in levels:
            if level < 15:
                self.face(level if level < bits else None)
            for bit in reversed(range(min(level, 14))):
                if self.spots[bit][0] == "l":
                    if level == bits and bit < 7 and self.spots[7][0] == "v":
                        self.swap()
                    yield
                    self.turn()
                if self.spots[bit][0] == "s":
                    self.swap()
                at = 1 << self.spots[bit][1]
                for low in range(16):
                    if not low & at:
                        exchange(self.keys, self.loads, low, low | at)
            if level == bits and self.spots[0][0] == "v":
                self.swap()


def run_all(takes):
    takes = list(takes)
    while takes:
        takes = [take for take in takes if next(take, takes) is not takes]


def sort_blocks(blocks, first):
    bits = 13 + len(blocks).bit_length()
    run_all(block.levels(range(first, min(bits, 14) + 1), bits) for block in blocks)
    for level in range(15, bits + 1):
        for block in blocks:
            block.face(level if level < bits else None)
        for bit in reversed(range(14, level)):
            for one in blocks:
                other = blocks[one.index | 1 << (bit - 14)]
                if other is not one:
                    for g in range(16):
                        exchange(one.keys, one.loads, g, g, other.keys, other.loads)
        run_all(block.levels([level], bits) for block in blocks)
    keys = sum((block.keys for block in blocks), [])
    return keys, sum((block.loads for block in blocks), [])


def lane_next(regs, fill):
    rolled = [pltpu.roll(x, LANES - 1, 1) for x in regs]
    rolled.append(jnp.full_like(rolled[0], fill))
    last = lane_iota() == LANES - 1
    return [jnp.where(last, rolled[h + 1], rolled[h]) for h in range(len(regs))]


def pull(regs, bit, linear):
    count = len(regs)
    blocks = count // 16
    kind, at = place(bit, linear)
    zero = jnp.zeros_like(regs[0])
    if kind == "s":
        step = 1 << at
        rolled = [pltpu.roll(x, ROWS - step, 0) for x in regs]
        stay = sub_iota() < ROWS - step
        if linear:
            over = rolled[1:] + [zero]
        else:
            wrap = lane_next([rolled[16 * h] for h in range(blocks)], 0)
            over = [rolled[g + 1] if (g + 1) % 16 else wrap[g // 16] for g in range(count)]
        return [jnp.where(stay, a, b) for a, b in zip(rolled, over)]
    step = 1 << at
    if linear or step >= 16:
        return regs[step:] + [zero] * step
    out = [None] * count
    for v in range(16):
        if v + step < 16:
            for h in range(blocks):
                out[16 * h + v] = regs[16 * h + v + step]
        else:
            wrap = lane_next([regs[16 * h + v + step - 16] for h in range(blocks)], 0)
            for h in range(blocks):
                out[16 * h + v] = wrap[h]
    return out


def push(regs, bit, linear):
    assert len(regs) == 16
    kind, at = place(bit, linear)
    zero = jnp.zeros_like(regs[0])
    first = lane_iota() == 0

    def lane_last(x):
        return jnp.where(first, 0, pltpu.roll(x, 1, 1))

    step = 1 << at
    if kind == "s":
        rolled = [pltpu.roll(x, step, 0) for x in regs]
        over = [zero if linear else lane_last(rolled[15])] + rolled[:15]
        stay = sub_iota() >= step
        return [jnp.where(stay, a, b) for a, b in zip(rolled, over)]
    head = [zero] * step if linear else [lane_last(x) for x in regs[16 - step :]]
    return head + regs[: 16 - step]


def spread_row(x, row):
    return jnp.broadcast_to(x[row : row + 1], (ROWS, LANES))


def down_lanes(row):
    return turned([row] * 16)


def over_rows(regs, op):
    while len(regs) > 1:
        regs = [op(a, b) for a, b in zip(regs[0::2], regs[1::2])]
    x = regs[0]
    for step in (4, 2, 1):
        x = op(x, pltpu.roll(x, step, 0))
    return x


def run_max(cells, keys):
    count = len(cells)
    blocks = count // 16
    sub = sub_iota()
    keys = list(keys)
    for step in (1, 2, 4):
        inside = sub >= step
        for g in range(count):
            same = (pltpu.roll(cells[g], step, 0) == cells[g]) & inside
            keys[g] = jnp.where(same, jnp.maximum(keys[g], pltpu.roll(keys[g], step, 0)), keys[g])
    for h in range(blocks):
        for v in range(1, 16):
            g = 16 * h + v
            cell, key = spread_row(cells[g - 1], 7), spread_row(keys[g - 1], 7)
            keys[g] = jnp.where(cells[g] == cell, jnp.maximum(keys[g], key), keys[g])
    last_cell = [spread_row(cells[16 * h + 15], 7) for h in range(blocks)]
    last_key = [spread_row(keys[16 * h + 15], 7) for h in range(blocks)]
    rolled = [jnp.full((ROWS, LANES), -9, jnp.int32)] + [pltpu.roll(x, 1, 1) for x in last_cell]
    lane = lane_iota()
    before = [jnp.where(lane == 0, rolled[h], rolled[h + 1]) for h in range(blocks)]
    cell_col = [down_lanes(x) for x in last_cell]
    key_col = [down_lanes(x) for x in last_key]
    for h in range(blocks):
        terms = []
        for source in range(h + 1):
            for v in range(16):
                match = cell_col[source][v] == before[h]
                if source == h:
                    match = match & (sub + ROWS * v < lane)
                terms.append((match, key_col[source][v]))
        terms = [jnp.where(match, key, -1) for match, key in terms]
        while len(terms) % 16 or len(terms) & (len(terms) - 1):
            terms.append(terms[0])
        best = over_rows(terms, jnp.maximum)
        for g in range(16 * h, 16 * h + 16):
            keys[g] = jnp.where(cells[g] == before[h], jnp.maximum(keys[g], best), keys[g])
    return keys


def run_ends(cells):
    count = len(cells)
    rolled = [pltpu.roll(x, ROWS - 1, 0) for x in cells]
    wrap = lane_next([rolled[16 * h] for h in range(count // 16)], -9)
    over = [rolled[g + 1] if (g + 1) % 16 else wrap[g // 16] for g in range(count)]
    bottom = sub_iota() == ROWS - 1
    return [c != jnp.where(bottom, b, a) for c, a, b in zip(cells, rolled, over)]


def ranks(flags):
    count = len(flags)
    blocks = count // 16
    sub, lane = sub_iota(), lane_iota()
    out, total = [], jnp.zeros((ROWS, LANES), jnp.int32)
    for h in range(blocks):
        sums, run = [], jnp.zeros((ROWS, LANES), jnp.int32)
        for v in range(16):
            flag = flags[16 * h + v]
            x = flag
            for step in (1, 2, 4):
                x = x + jnp.where(sub >= step, pltpu.roll(x, step, 0), 0)
            sums.append(x - flag + run)
            run = run + spread_row(x, 7)
        col = down_lanes(run)
        start = [jnp.where(sub + ROWS * v < lane, col[v], 0) for v in range(16)]
        start = over_rows(start, jnp.add) + total
        total = total + over_rows(col, jnp.add)
        out += [x + start for x in sums]
    return out, total


def positions(count, linear):
    sub, lane = sub_iota(), lane_iota()
    if linear:
        return [TILE * g + LANES * sub + lane for g in range(count)]
    return [BLOCK * (g // 16) + LANES * lane + ROWS * (g % 16) + sub for g in range(count)]


def travel(move, load, bit, linear, shift, empty):
    probe = 1 << (CUT + bit)
    new_move, new_load = shift(move, bit, linear), shift(load, bit, linear)
    for g in range(len(move)):
        arrives = (new_move[g] & probe) != 0
        old_move, old_load = move[g], load[g]
        if empty is not None:
            leaves = (old_move & probe) != 0
            old_move, old_load = jnp.where(leaves, 0, old_move), jnp.where(leaves, empty, old_load)
        new_move[g] = jnp.where(arrives, new_move[g], old_move)
        new_load[g] = jnp.where(arrives, new_load[g], old_load)
    return new_move, new_load


def compact(cells, keys, wanted):
    count = len(cells)
    rank, total = ranks([jnp.where(w, 1, 0) for w in wanted])
    at = positions(count, False)
    move = [
        jnp.where(w, (i - r) << CUT | c, 0) for w, i, r, c in zip(wanted, at, rank, cells)
    ]
    for bit in range((count * TILE).bit_length() - 1):
        if bit == 7:
            move, keys = turned(move), turned(keys)
        move, keys = travel(move, keys, bit, bit >= 7, pull, None)
    return [x & LOW for x in move], keys, total


def owner_sizes(flags, cells, n, shift):
    sums = [jnp.zeros((ROWS, LANES), jnp.int32)] * (n // 4)
    for w, c in zip(flags, cells):
        group = jnp.where(w, c >> (shift + 2), -1)
        unit = jnp.left_shift(1, (c >> (shift - 3)) & 24)
        sums = [x + jnp.where(group == k, unit, 0) for k, x in enumerate(sums)]
    sizes = []
    for x in sums:
        pairs = []
        for part in (x & 0xFF00FF, (x >> 8) & 0xFF00FF):
            for step in (4, 2, 1):
                part = part + pltpu.roll(part, step, 0)
            pairs.append(part)
        for half in (0, 16):
            for part in pairs:
                row = (part >> half) & 0xFFFF
                sizes.append(jnp.sum(jnp.where(sub_iota() == 0, row, 0)))
    return sizes


def split_kernel(own, slots, chunk, round_ref, odd_ref, cell_in, vehicle_in, speed_in, out_hbm, cell_ref, vehicle_ref, speed_ref, out_ref, low_ref, high_ref, cell_pad, key_pad, in_sem, out_sem):
    n = CELLS // own
    count = cell_ref.shape[0] // ROWS
    bits = (count * TILE).bit_length() - 1
    odd = odd_ref[0]
    arrays = ((cell_in, cell_ref), (vehicle_in, vehicle_ref), (speed_in, speed_ref))
    copies = []
    for h in range(count // 16):
        part = pl.ds(LANES * h, LANES)
        copies.append(
            [
                pltpu.make_async_copy(x.at[part, :], y.at[part, :], in_sem.at[h, k])
                for k, (x, y) in enumerate(arrays)
            ]
        )
        for copy in copies[h]:
            copy.start()
    blocks = []
    for h in range(count // 16):
        for copy in copies[h]:
            copy.wait()
        some_cells, some_keys = [], []
        for g in range(16 * h, 16 * h + 16):
            at = pl.ds(ROWS * g, ROWS)
            cell = cell_ref[at, :]
            some_cells.append(jnp.where(odd == 1, CELLS - 1 - cell, cell))
            level = (speed_ref[at, :] * float(STEPS)).astype(jnp.int32)
            some_keys.append(level * VEHICLES + (VEHICLES - 1 - vehicle_ref[at, :]))
        block = Block(lambda: (some_cells, some_keys), h, False, cell_pad, key_pad)
        run_all([block.levels(range(1, 8), bits)])
        blocks.append(block)
    cells, keys = sort_blocks(blocks, 8)
    keys = run_max(cells, keys)
    ends = run_ends(cells)
    shift = own.bit_length() - 1
    sizes = owner_sizes(ends, cells, n, shift)
    high = [k | (c >> CUT) << 27 for k, c in zip(keys, cells)]
    low, high, _ = compact([c & LOW for c in cells], high, ends)
    for g in range(count):
        at = pl.ds(ROWS * g, ROWS)
        low_ref[at, :] = low[g]
        high_ref[at, :] = high[g]
    low_ref[pl.ds(ROWS * count, ROWS), :] = jnp.zeros((ROWS, LANES), jnp.int32)
    high_ref[pl.ds(ROWS * count, ROWS), :] = jnp.zeros((ROWS, LANES), jnp.int32)
    most = functools.reduce(jnp.maximum, sizes)
    sub, lane = sub_iota(), lane_iota()
    skip = round_ref[0] * (slots * LANES)
    base = jnp.int32(0)
    group = n // 4
    writes = []
    for k in range(4):
        part = pl.ds(jnp.where(odd == 1, 3 - k, k) * (group * chunk), group * chunk)
        writes.append(
            pltpu.make_async_copy(out_ref.at[part, :], out_hbm.at[part, :], out_sem.at[k])
        )
    for o in range(n):
        if o % group == 0 and o > group:
            writes[o // group - 2].start()
        start = base + skip
        valid = sub * LANES + lane < sizes[o] - skip
        start = jnp.minimum(start, count * TILE)
        base = base + sizes[o]
        row, off = start >> 7, start & 127

        def window(ref):
            x = pltpu.roll(ref[pl.ds(row, ROWS), :], (LANES - off) & 127, 1)
            return jnp.where(lane < LANES - off, x, pltpu.roll(x, ROWS - 1, 0))

        low_w, high_w = window(low_ref), window(high_ref)
        cell = jnp.where(valid, low_w & (own - 1), own).astype(jnp.float32)
        level = (high_w & ((1 << 27) - 1)) >> 10
        speed = level.astype(jnp.float32) * (1.0 / STEPS)
        ident = (~high_w & (VEHICLES - 1)).astype(jnp.float32)
        target = pl.multiple_of(jnp.where(odd == 1, n - 1 - o, o) * chunk, chunk)
        for w, x in enumerate((cell, speed, ident)):
            out_ref[pl.ds(target + w * slots, slots), :] = x[:slots]
        tail = chunk - 3 * slots
        fill = jnp.full((tail, LANES), most.astype(jnp.float32))
        out_ref[pl.ds(target + 3 * slots, tail), :] = fill
    for k in (2, 3):
        writes[k].start()
    for write in writes:
        write.wait()


def join_kernel(own, n, slots, chunk, in_ref, speed_ref, ident_ref, rounds_ref, cell_pad, key_pad):
    sub = sub_iota()
    per = ROWS // run_rows(slots)

    def load(h):
        cells, keys = [], []
        late = jnp.where(blocks[h - 1].loads[15] > 1 << 30, 1, 0) if h else 0
        for g in range(16 * h, 16 * h + 16):
            if per == 1:
                part = [in_ref[pl.ds(chunk * g + w * slots, slots), :] for w in range(3)]
                pad = jnp.zeros((ROWS - slots, LANES), jnp.float32)
                part = [jnp.concatenate([x, pad], axis=0) for x in part]
                cell = jnp.where(sub < slots, part[0].astype(jnp.int32), own)
                cell = own - 1 - cell if g & 1 else cell
            else:
                part = [
                    in_ref[pl.ds(chunk * per * g + w, ROWS, stride=chunk), :] for w in range(3)
                ]
                cell = part[0].astype(jnp.int32)
                cell = jnp.where(sub & 1 == 1, own - 1 - cell, cell)
            level = (part[1] * float(STEPS)).astype(jnp.int32)
            cells.append(cell + late)
            keys.append(level * VEHICLES + (VEHICLES - 1 - part[2].astype(jnp.int32)))
        return cells, keys

    most = jnp.zeros((ROWS, LANES), jnp.float32)
    for source in range(n):
        most = jnp.maximum(most, in_ref[pl.ds(chunk * (source + 1) - ROWS, ROWS), :])
    most = jnp.max(jnp.where(sub == ROWS - 1, most, 0.0)).astype(jnp.int32)
    rounds_ref[0] = lax.div(most + (slots * LANES - 1), jnp.int32(slots * LANES))
    first = (run_rows(slots) * LANES).bit_length()
    blocks = [
        Block(functools.partial(load, h), h, True, cell_pad, key_pad) for h in range(n // per // 16)
    ]
    cells, keys = sort_blocks(blocks, first)
    keys = run_max(cells, keys)
    ends = [w & (c >= 0) & (c < own) for w, c in zip(run_ends(cells), cells)]
    cells, keys, total = compact(cells, keys, ends)
    keep = max(own // TILE, 1)
    at = positions(16, True)
    move = [jnp.where(i < total, (c - i) << CUT, 0) for i, c in zip(at, cells)]
    keys = [jnp.where(i < total, k, -1) for i, k in zip(at, keys)]
    linear = True
    for bit in reversed(range(own.bit_length() - 1)):
        if bit == 6:
            move, keys, linear = turned(move), turned(keys), False
        move, keys = travel(move, keys, bit, linear, push, -1)
    keys = turned(keys)
    for g in range(keep):
        key = keys[g]
        at = pl.ds(ROWS * g, ROWS)
        speed = (key >> 10).astype(jnp.float32) * (1.0 / STEPS)
        speed_ref[at, :] = jnp.where(key >= 0, speed, -1.0)
        ident_ref[at, :] = jnp.where(key >= 0, VEHICLES - 1 - (key & (VEHICLES - 1)), -1)


def run_rows(slots):
    return 1 << (slots - 1).bit_length()


def pads(rows):
    return [pltpu.VMEM((rows // ROWS * PITCH, LANES), jnp.int32)] * 2


def per_device(cell, vehicle, speed):
    n = lax.axis_size(AXES)
    own = CELLS // n
    events = cell.shape[0]
    slots = max(1, (5 * events // n) // (8 * LANES))
    chunk = -(-(3 * slots + 1) // ROWS) * ROWS
    rows = events // LANES
    smem = pl.BlockSpec(memory_space=pltpu.SMEM)
    vmem = pl.BlockSpec(memory_space=pltpu.VMEM)
    hbm = pl.BlockSpec(memory_space=pl.ANY)
    params = pltpu.CompilerParams(vmem_limit_bytes=16 << 20)
    table = (own // LANES, LANES)
    odd = (lax.axis_index(AXES) & 1).reshape(1)
    inputs = [x.reshape(rows, LANES) for x in (cell, vehicle, speed)]

    split = pl.pallas_call(
        functools.partial(split_kernel, own, slots, chunk),
        out_shape=jax.ShapeDtypeStruct((n * chunk, LANES), jnp.float32),
        in_specs=[smem, smem, hbm, hbm, hbm],
        out_specs=hbm,
        scratch_shapes=[
            pltpu.VMEM((rows, LANES), jnp.int32),
            pltpu.VMEM((rows, LANES), jnp.int32),
            pltpu.VMEM((rows, LANES), jnp.float32),
            pltpu.VMEM((n * chunk, LANES), jnp.float32),
            pltpu.VMEM((rows + ROWS, LANES), jnp.int32),
            pltpu.VMEM((rows + ROWS, LANES), jnp.int32),
        ]
        + pads(rows)
        + [pltpu.SemaphoreType.DMA((rows // LANES, 3)), pltpu.SemaphoreType.DMA((4,))],
        compiler_params=params,
        name="split",
    )
    join = pl.pallas_call(
        functools.partial(join_kernel, own, n, slots, chunk),
        out_shape=(
            jax.ShapeDtypeStruct(table, jnp.float32),
            jax.ShapeDtypeStruct(table, jnp.int32),
            jax.ShapeDtypeStruct((1,), jnp.int32),
        ),
        in_specs=[vmem],
        out_specs=(vmem, vmem, smem),
        scratch_shapes=pads(n * run_rows(slots)),
        compiler_params=params,
        name="join",
    )

    def one_round(index):
        sent = split(index.reshape(1), odd, *inputs)
        got = lax.all_to_all(sent.reshape(n, chunk, LANES), AXES, 0, 0, tiled=True)
        return join(got.reshape(n * chunk, LANES))

    best, ident, rounds = one_round(jnp.int32(0))

    def again(state):
        index, best, ident = state
        more, other, _ = one_round(index)
        ident = jnp.where(
            more > best, other, jnp.where(more < best, ident, jnp.minimum(ident, other))
        )
        return index + 1, jnp.maximum(best, more), ident

    _, best, ident = lax.while_loop(
        lambda state: state[0] < rounds[0], again, (jnp.int32(1), best, ident)
    )
    return best.reshape(own), ident.reshape(own)


def solution(mesh):
    placed = P(AXES)
    return jax.shard_map(
        per_device,
        mesh=mesh,
        in_specs=(placed, placed, placed),
        out_specs=(placed, placed),
        check_vma=False,
    )
```

```python
import functools

import jax
import jax.numpy as jnp
from jax import lax
from jax.experimental import pallas as pl
from jax.experimental.pallas import tpu as pltpu
from jax.sharding import PartitionSpec as P

CELLS = 524288
VEHICLES = 1024
STEPS = 1024
AXES = ("gx", "gy")
LANES = 128
ROWS = 8
TILE = ROWS * LANES
BLOCK = LANES * LANES
CUT = 15
LOW = (1 << CUT) - 1
PITCH = ROWS + 1


def sub_iota():
    return lax.broadcasted_iota(jnp.int32, (ROWS, LANES), 0)


def lane_iota():
    return lax.broadcasted_iota(jnp.int32, (ROWS, LANES), 1)


def turned(regs):
    out = []
    for first in range(0, len(regs), 16):
        block = jnp.concatenate(regs[first : first + 16], axis=0).T
        out += [block[ROWS * i : ROWS * (i + 1)] for i in range(16)]
    return out


def place(bit, linear):
    if bit >= 14:
        return "v", bit - 10
    if linear:
        return ("l", bit) if bit < 7 else ("s", bit - 7) if bit < 10 else ("v", bit - 10)
    return ("s", bit) if bit < 3 else ("v", bit - 3) if bit < 7 else ("l", bit - 7)


def swapped(regs, ref):
    for g, x in enumerate(regs):
        ref[pl.ds(PITCH * g, ROWS), :] = x
    return [
        ref[pl.ds(PITCH * (g & ~7) + (g & 7), ROWS, stride=PITCH), :] for g in range(len(regs))
    ]


def exchange(keys, loads, low, high, more_keys=None, more_loads=None):
    more_keys = keys if more_keys is None else more_keys
    more_loads = loads if more_loads is None else more_loads
    a, b, p, q = keys[low], more_keys[high], loads[low], more_loads[high]
    larger = a > b
    keys[low], more_keys[high] = jnp.minimum(a, b), jnp.maximum(a, b)
    loads[low], more_loads[high] = jnp.where(larger, q, p), jnp.where(larger, p, q)


class Block:
    def __init__(self, load, index, linear, key_ref, load_ref):
        self.load, self.index = load, index
        self.spots = [place(bit, linear) for bit in range(14)]
        at = pl.ds(16 * PITCH * index, 16 * PITCH)
        self.refs = key_ref.at[at, :], load_ref.at[at, :]
        self.faced = None

    def moved(self, pairs, change):
        names = dict(pairs) | {b: a for a, b in pairs}
        self.spots = [names.get(spot, spot) for spot in self.spots]
        self.keys = change(self.keys, self.refs[0])
        self.loads = change(self.loads, self.refs[1])

    def turn(self):
        pairs = [(("s", b), ("l", b)) for b in range(3)]
        pairs += [(("v", b), ("l", b + 3)) for b in range(4)]
        self.moved(pairs, lambda regs, ref: turned(regs))

    def swap(self):
        self.moved([(("s", b), ("v", b)) for b in range(3)], swapped)

    def face(self, bit):
        odd, mask = [0] * 16, None
        for each in {self.faced, bit} - {None}:
            kind, at = self.spots[each] if each < 14 else ("h", each - 14)
            if kind == "h":
                odd = [x ^ (self.index >> at & 1) for x in odd]
            elif kind == "v":
                odd = [x ^ (g >> at & 1) for g, x in enumerate(odd)]
            else:
                index = sub_iota() if kind == "s" else lane_iota()
                one = -((index >> at) & 1)
                mask = one if mask is None else mask ^ one
        if mask is None:
            self.keys = [~x if o else x for x, o in zip(self.keys, odd)]
        else:
            masks = mask, ~mask
            self.keys = [x ^ masks[o] for x, o in zip(self.keys, odd)]
        self.faced = bit

    def levels(self, levels, bits):
        if self.load is not None:
            self.keys, self.loads = self.load()
            self.load = None
        for level in levels:
            if level < 15:
                self.face(level if level < bits else None)
            for bit in reversed(range(min(level, 14))):
                if self.spots[bit][0] == "l":
                    if level == bits and bit < 7 and self.spots[7][0] == "v":
                        self.swap()
                    yield
                    self.turn()
                if self.spots[bit][0] == "s":
                    self.swap()
                at = 1 << self.spots[bit][1]
                for low in range(16):
                    if not low & at:
                        exchange(self.keys, self.loads, low, low | at)


def run_all(takes):
    takes = list(takes)
    while takes:
        takes = [take for take in takes if next(take, takes) is not takes]


def sort_blocks(blocks, first):
    bits = 13 + len(blocks).bit_length()
    run_all(block.levels(range(first, min(bits, 14) + 1), bits) for block in blocks)
    for level in range(15, bits + 1):
        for block in blocks:
            block.face(level if level < bits else None)
        for bit in reversed(range(14, level)):
            for one in blocks:
                other = blocks[one.index | 1 << (bit - 14)]
                if other is not one:
                    for g in range(16):
                        exchange(one.keys, one.loads, g, g, other.keys, other.loads)
        run_all(block.levels([level], bits) for block in blocks)
    keys = sum((block.keys for block in blocks), [])
    return keys, sum((block.loads for block in blocks), [])


def lane_next(regs, fill):
    rolled = [pltpu.roll(x, LANES - 1, 1) for x in regs]
    rolled.append(jnp.full_like(rolled[0], fill))
    last = lane_iota() == LANES - 1
    return [jnp.where(last, rolled[h + 1], rolled[h]) for h in range(len(regs))]


def pull(regs, bit, linear):
    count = len(regs)
    blocks = count // 16
    kind, at = place(bit, linear)
    zero = jnp.zeros_like(regs[0])
    if kind == "s":
        step = 1 << at
        rolled = [pltpu.roll(x, ROWS - step, 0) for x in regs]
        stay = sub_iota() < ROWS - step
        if linear:
            over = rolled[1:] + [zero]
        else:
            wrap = lane_next([rolled[16 * h] for h in range(blocks)], 0)
            over = [rolled[g + 1] if (g + 1) % 16 else wrap[g // 16] for g in range(count)]
        return [jnp.where(stay, a, b) for a, b in zip(rolled, over)]
    step = 1 << at
    if linear or step >= 16:
        return regs[step:] + [zero] * step
    out = [None] * count
    for v in range(16):
        if v + step < 16:
            for h in range(blocks):
                out[16 * h + v] = regs[16 * h + v + step]
        else:
            wrap = lane_next([regs[16 * h + v + step - 16] for h in range(blocks)], 0)
            for h in range(blocks):
                out[16 * h + v] = wrap[h]
    return out


def pull_woven(regs, bit, linear):
    step = 1 << bit
    out = list(regs[step:]) + [None] * step
    bottom = sub_iota() == ROWS - 1
    for v in range(8 - step, 8):
        rolled = [pltpu.roll(x, ROWS - 1, 0) for x in regs[v + step - 8 :: 8]]
        wrap = lane_next(rolled[0::2], 0)
        for c, x in enumerate(rolled):
            out[8 * c + v] = jnp.where(bottom, wrap[c // 2] if c & 1 else rolled[c + 1], x)
    return out


def push(regs, bit, linear):
    assert len(regs) == 16
    kind, at = place(bit, linear)
    zero = jnp.zeros_like(regs[0])
    first = lane_iota() == 0

    def lane_last(x):
        return jnp.where(first, 0, pltpu.roll(x, 1, 1))

    step = 1 << at
    if kind == "s":
        rolled = [pltpu.roll(x, step, 0) for x in regs]
        over = [zero if linear else lane_last(rolled[15])] + rolled[:15]
        stay = sub_iota() >= step
        return [jnp.where(stay, a, b) for a, b in zip(rolled, over)]
    head = [zero] * step if linear else [lane_last(x) for x in regs[16 - step :]]
    return head + regs[: 16 - step]


def spread_row(x, row):
    return jnp.broadcast_to(x[row : row + 1], (ROWS, LANES))


def down_lanes(row):
    return turned([row] * 16)


def over_rows(regs, op):
    while len(regs) > 1:
        regs = [op(a, b) for a, b in zip(regs[0::2], regs[1::2])]
    x = regs[0]
    for step in (4, 2, 1):
        x = op(x, pltpu.roll(x, step, 0))
    return x


def run_max(cells, keys):
    count = len(cells)
    blocks = count // 16
    sub, lane = sub_iota(), lane_iota()
    keys = list(keys)

    def carry(g, cell, key, also=None):
        same = cells[g] == cell
        same = same if also is None else same & also
        keys[g] = jnp.where(same, jnp.maximum(keys[g], key), keys[g])

    for g in range(count):
        if g % 8:
            carry(g, cells[g - 1], keys[g - 1])
    ends = range(7, count, 8)
    final = [keys[g] for g in ends]
    last = [cells[g] for g in ends]

    def join(c, cell, key, also=None):
        same = last[c] == cell
        same = same if also is None else same & also
        final[c] = jnp.where(same, jnp.maximum(final[c], key), final[c])

    for step in (1, 2, 4):
        for c in range(len(last)):
            join(c, pltpu.roll(last[c], step, 0), pltpu.roll(final[c], step, 0), sub >= step)
    for c in range(1, len(last), 2):
        join(c, spread_row(last[c - 1], 7), spread_row(final[c - 1], 7))
    last_cell = [spread_row(x, 7) for x in last[1::2]]
    last_key = [spread_row(x, 7) for x in final[1::2]]
    rolled = [jnp.full((ROWS, LANES), -9, jnp.int32)] + [pltpu.roll(x, 1, 1) for x in last_cell]
    before = [jnp.where(lane == 0, rolled[h], rolled[h + 1]) for h in range(blocks)]
    cell_col = [down_lanes(x) for x in last_cell]
    key_col = [down_lanes(x) for x in last_key]
    for h in range(blocks):
        terms = []
        for source in range(h + 1):
            for v in range(16):
                match = cell_col[source][v] == before[h]
                if source == h:
                    match = match & (sub + ROWS * v < lane)
                terms.append(jnp.where(match, key_col[source][v], -1))
        while len(terms) & (len(terms) - 1):
            terms.append(terms[0])
        best = over_rows(terms, jnp.maximum)
        for c in (2 * h, 2 * h + 1):
            join(c, before[h], best)
            cell, key = before[h], best
            if c & 1:
                cell, key = spread_row(last[c - 1], 7), spread_row(final[c - 1], 7)
            cell = jnp.where(sub == 0, cell, pltpu.roll(last[c], 1, 0))
            key = jnp.where(sub == 0, key, pltpu.roll(final[c], 1, 0))
            for g in range(8 * c, 8 * c + 8):
                carry(g, cell, key)
    return keys


def run_ends(cells):
    count = len(cells)
    bottom = sub_iota() == ROWS - 1
    rolled = [pltpu.roll(x, ROWS - 1, 0) for x in cells[::8]]
    wrap = lane_next(rolled[::2], -9)
    out = []
    for g in range(count):
        c = g // 8
        if g % 8 < 7:
            after = cells[g + 1]
        else:
            after = jnp.where(bottom, wrap[c // 2] if c & 1 else rolled[c + 1], rolled[c])
        out.append(cells[g] != after)
    return out


def ranks(flags):
    count = len(flags)
    sub, lane = sub_iota(), lane_iota()
    out, total = [], jnp.zeros((ROWS, LANES), jnp.int32)
    for h in range(count // 16):
        starts, run = [], jnp.zeros((ROWS, LANES), jnp.int32)
        for c in (2 * h, 2 * h + 1):
            here = jnp.zeros((ROWS, LANES), jnp.int32)
            for g in range(8 * c, 8 * c + 8):
                out.append(here)
                here = here + flags[g]
            x = here
            for step in (1, 2, 4):
                x = x + jnp.where(sub >= step, pltpu.roll(x, step, 0), 0)
            starts.append(x - here + run)
            run = run + spread_row(x, 7)
        col = down_lanes(run)
        start = [jnp.where(sub + ROWS * v < lane, col[v], 0) for v in range(16)]
        start = over_rows(start, jnp.add) + total
        total = total + over_rows(col, jnp.add)
        starts = [x + start for x in starts]
        for g in range(16 * h, 16 * h + 16):
            out[g] = out[g] + starts[g // 8 % 2]
    return out, total


def positions(count, linear):
    sub, lane = sub_iota(), lane_iota()
    if linear:
        return [TILE * g + LANES * sub + lane for g in range(count)]
    weave = LANES * lane + ROWS * sub
    return [weave + (BLOCK * (g // 16) + 64 * (g // 8 % 2) + g % 8) for g in range(count)]


def travel(move, load, bit, linear, shift, empty):
    probe = 1 << (CUT + bit)
    new_move, new_load = shift(move, bit, linear), shift(load, bit, linear)
    for g in range(len(move)):
        arrives = (new_move[g] & probe) != 0
        old_move, old_load = move[g], load[g]
        if empty is not None:
            leaves = (old_move & probe) != 0
            old_move, old_load = jnp.where(leaves, 0, old_move), jnp.where(leaves, empty, old_load)
        new_move[g] = jnp.where(arrives, new_move[g], old_move)
        new_load[g] = jnp.where(arrives, new_load[g], old_load)
    return new_move, new_load


def compact(cells, keys, wanted, cell_ref, key_ref):
    count = len(cells)
    rank, total = ranks([jnp.where(w, 1, 0) for w in wanted])
    at = positions(count, False)
    move = [
        jnp.where(w, (i - r) << CUT | c, 0) for w, i, r, c in zip(wanted, at, rank, cells)
    ]
    for bit in range((count * TILE).bit_length() - 1):
        if bit == 3:
            move, keys = swapped(move, cell_ref), swapped(keys, key_ref)
        if bit == 7:
            move, keys = turned(move), turned(keys)
        move, keys = travel(move, keys, bit, bit >= 7, pull if bit >= 3 else pull_woven, None)
    return [x & LOW for x in move], keys, total


def owner_sizes(flags, cells, n, shift):
    sums = [jnp.zeros((ROWS, LANES), jnp.int32)] * (n // 4)
    for w, c in zip(flags, cells):
        group = jnp.where(w, c >> (shift + 2), -1)
        unit = jnp.left_shift(1, (c >> (shift - 3)) & 24)
        sums = [x + jnp.where(group == k, unit, 0) for k, x in enumerate(sums)]
    sizes = []
    for x in sums:
        pairs = []
        for part in (x & 0xFF00FF, (x >> 8) & 0xFF00FF):
            for step in (4, 2, 1):
                part = part + pltpu.roll(part, step, 0)
            pairs.append(part)
        for half in (0, 16):
            for part in pairs:
                row = (part >> half) & 0xFFFF
                sizes.append(jnp.sum(jnp.where(sub_iota() == 0, row, 0)))
    return sizes


def split_kernel(own, slots, chunk, round_ref, odd_ref, cell_in, vehicle_in, speed_in, out_hbm, cell_ref, vehicle_ref, speed_ref, out_ref, low_ref, high_ref, cell_pad, key_pad, in_sem, out_sem):
    n = CELLS // own
    count = cell_ref.shape[0] // ROWS
    bits = (count * TILE).bit_length() - 1
    odd = odd_ref[0]
    arrays = ((cell_in, cell_ref), (vehicle_in, vehicle_ref), (speed_in, speed_ref))
    copies = []
    for h in range(count // 16):
        part = pl.ds(LANES * h, LANES)
        copies.append(
            [
                pltpu.make_async_copy(x.at[part, :], y.at[part, :], in_sem.at[h, k])
                for k, (x, y) in enumerate(arrays)
            ]
        )
        for copy in copies[h]:
            copy.start()
    blocks = []
    for h in range(count // 16):
        for copy in copies[h]:
            copy.wait()
        some_cells, some_keys = [], []
        for g in range(16 * h, 16 * h + 16):
            at = pl.ds(ROWS * g, ROWS)
            cell = cell_ref[at, :]
            some_cells.append(jnp.where(odd == 1, CELLS - 1 - cell, cell))
            level = (speed_ref[at, :] * float(STEPS)).astype(jnp.int32)
            some_keys.append(level * VEHICLES + (VEHICLES - 1 - vehicle_ref[at, :]))
        block = Block(lambda: (some_cells, some_keys), h, False, cell_pad, key_pad)
        run_all([block.levels(range(1, 8), bits)])
        blocks.append(block)
    cells, keys = sort_blocks(blocks, 8)
    keys = run_max(cells, keys)
    ends = run_ends(cells)
    shift = own.bit_length() - 1
    sizes = owner_sizes(ends, cells, n, shift)
    high = [k | (c >> CUT) << 27 for k, c in zip(keys, cells)]
    low, high, _ = compact([c & LOW for c in cells], high, ends, cell_pad, key_pad)
    for g in range(count):
        at = pl.ds(ROWS * g, ROWS)
        low_ref[at, :] = low[g]
        high_ref[at, :] = high[g]
    low_ref[pl.ds(ROWS * count, ROWS), :] = jnp.zeros((ROWS, LANES), jnp.int32)
    high_ref[pl.ds(ROWS * count, ROWS), :] = jnp.zeros((ROWS, LANES), jnp.int32)
    most = functools.reduce(jnp.maximum, sizes)
    sub, lane = sub_iota(), lane_iota()
    skip = round_ref[0] * (slots * LANES)
    base = jnp.int32(0)
    group = n // 4
    writes = []
    for k in range(4):
        part = pl.ds(jnp.where(odd == 1, 3 - k, k) * (group * chunk), group * chunk)
        writes.append(
            pltpu.make_async_copy(out_ref.at[part, :], out_hbm.at[part, :], out_sem.at[k])
        )
    for o in range(n):
        if o % group == 0 and o > group:
            writes[o // group - 2].start()
        start = base + skip
        valid = sub * LANES + lane < sizes[o] - skip
        start = jnp.minimum(start, count * TILE)
        base = base + sizes[o]
        row, off = start >> 7, start & 127

        def window(ref):
            x = pltpu.roll(ref[pl.ds(row, ROWS), :], (LANES - off) & 127, 1)
            return jnp.where(lane < LANES - off, x, pltpu.roll(x, ROWS - 1, 0))

        low_w, high_w = window(low_ref), window(high_ref)
        cell = jnp.where(valid, low_w & (own - 1), own).astype(jnp.float32)
        level = (high_w & ((1 << 27) - 1)) >> 10
        speed = level.astype(jnp.float32) * (1.0 / STEPS)
        ident = (~high_w & (VEHICLES - 1)).astype(jnp.float32)
        target = pl.multiple_of(jnp.where(odd == 1, n - 1 - o, o) * chunk, chunk)
        for w, x in enumerate((cell, speed, ident)):
            out_ref[pl.ds(target + w * slots, slots), :] = x[:slots]
        tail = chunk - 3 * slots
        fill = jnp.full((tail, LANES), most.astype(jnp.float32))
        out_ref[pl.ds(target + 3 * slots, tail), :] = fill
    for k in (2, 3):
        writes[k].start()
    for write in writes:
        write.wait()


def join_kernel(own, n, slots, chunk, in_ref, speed_ref, ident_ref, rounds_ref, cell_pad, key_pad):
    sub = sub_iota()
    per = ROWS // run_rows(slots)

    def load(h):
        cells, keys = [], []
        late = jnp.where(blocks[h - 1].loads[15] > 1 << 30, 1, 0) if h else 0
        for g in range(16 * h, 16 * h + 16):
            if per == 1:
                part = [in_ref[pl.ds(chunk * g + w * slots, slots), :] for w in range(3)]
                pad = jnp.zeros((ROWS - slots, LANES), jnp.float32)
                part = [jnp.concatenate([x, pad], axis=0) for x in part]
                cell = jnp.where(sub < slots, part[0].astype(jnp.int32), own)
                cell = own - 1 - cell if g & 1 else cell
            else:
                part = [
                    in_ref[pl.ds(chunk * per * g + w, ROWS, stride=chunk), :] for w in range(3)
                ]
                cell = part[0].astype(jnp.int32)
                cell = jnp.where(sub & 1 == 1, own - 1 - cell, cell)
            level = (part[1] * float(STEPS)).astype(jnp.int32)
            cells.append(cell + late)
            keys.append(level * VEHICLES + (VEHICLES - 1 - part[2].astype(jnp.int32)))
        return cells, keys

    most = jnp.zeros((ROWS, LANES), jnp.float32)
    for source in range(n):
        most = jnp.maximum(most, in_ref[pl.ds(chunk * (source + 1) - ROWS, ROWS), :])
    most = jnp.max(jnp.where(sub == ROWS - 1, most, 0.0)).astype(jnp.int32)
    rounds_ref[0] = lax.div(most + (slots * LANES - 1), jnp.int32(slots * LANES))
    first = (run_rows(slots) * LANES).bit_length()
    blocks = [
        Block(functools.partial(load, h), h, True, cell_pad, key_pad) for h in range(n // per // 16)
    ]
    cells, keys = sort_blocks(blocks, first)
    keys = run_max(cells, keys)
    ends = [w & (c >= 0) & (c < own) for w, c in zip(run_ends(cells), cells)]
    cells, keys, total = compact(cells, keys, ends, cell_pad, key_pad)
    keep = max(own // TILE, 1)
    at = positions(16, True)
    move = [jnp.where(i < total, (c - i) << CUT, 0) for i, c in zip(at, cells)]
    keys = [jnp.where(i < total, k, -1) for i, k in zip(at, keys)]
    linear = True
    for bit in reversed(range(own.bit_length() - 1)):
        if bit == 6:
            move, keys, linear = turned(move), turned(keys), False
        move, keys = travel(move, keys, bit, linear, push, -1)
    keys = turned(keys)
    for g in range(keep):
        key = keys[g]
        at = pl.ds(ROWS * g, ROWS)
        speed = (key >> 10).astype(jnp.float32) * (1.0 / STEPS)
        speed_ref[at, :] = jnp.where(key >= 0, speed, -1.0)
        ident_ref[at, :] = jnp.where(key >= 0, VEHICLES - 1 - (key & (VEHICLES - 1)), -1)


def run_rows(slots):
    return 1 << (slots - 1).bit_length()


def pads(rows):
    return [pltpu.VMEM((rows // ROWS * PITCH, LANES), jnp.int32)] * 2


def per_device(cell, vehicle, speed):
    n = lax.axis_size(AXES)
    own = CELLS // n
    events = cell.shape[0]
    slots = max(1, (5 * events // n) // (8 * LANES))
    chunk = -(-(3 * slots + 1) // ROWS) * ROWS
    rows = events // LANES
    smem = pl.BlockSpec(memory_space=pltpu.SMEM)
    vmem = pl.BlockSpec(memory_space=pltpu.VMEM)
    hbm = pl.BlockSpec(memory_space=pl.ANY)
    params = pltpu.CompilerParams(vmem_limit_bytes=16 << 20)
    table = (own // LANES, LANES)
    odd = (lax.axis_index(AXES) & 1).reshape(1)
    inputs = [x.reshape(rows, LANES) for x in (cell, vehicle, speed)]

    split = pl.pallas_call(
        functools.partial(split_kernel, own, slots, chunk),
        out_shape=jax.ShapeDtypeStruct((n * chunk, LANES), jnp.float32),
        in_specs=[smem, smem, hbm, hbm, hbm],
        out_specs=hbm,
        scratch_shapes=[
            pltpu.VMEM((rows, LANES), jnp.int32),
            pltpu.VMEM((rows, LANES), jnp.int32),
            pltpu.VMEM((rows, LANES), jnp.float32),
            pltpu.VMEM((n * chunk, LANES), jnp.float32),
            pltpu.VMEM((rows + ROWS, LANES), jnp.int32),
            pltpu.VMEM((rows + ROWS, LANES), jnp.int32),
        ]
        + pads(rows)
        + [pltpu.SemaphoreType.DMA((rows // LANES, 3)), pltpu.SemaphoreType.DMA((4,))],
        compiler_params=params,
        name="split",
    )
    join = pl.pallas_call(
        functools.partial(join_kernel, own, n, slots, chunk),
        out_shape=(
            jax.ShapeDtypeStruct(table, jnp.float32),
            jax.ShapeDtypeStruct(table, jnp.int32),
            jax.ShapeDtypeStruct((1,), jnp.int32),
        ),
        in_specs=[vmem],
        out_specs=(vmem, vmem, smem),
        scratch_shapes=pads(n * run_rows(slots)),
        compiler_params=params,
        name="join",
    )

    def one_round(index):
        sent = split(index.reshape(1), odd, *inputs)
        got = lax.all_to_all(sent.reshape(n, chunk, LANES), AXES, 0, 0, tiled=True)
        return join(got.reshape(n * chunk, LANES))

    best, ident, rounds = one_round(jnp.int32(0))

    def again(state):
        index, best, ident = state
        more, other, _ = one_round(index)
        ident = jnp.where(
            more > best, other, jnp.where(more < best, ident, jnp.minimum(ident, other))
        )
        return index + 1, jnp.maximum(best, more), ident

    _, best, ident = lax.while_loop(
        lambda state: state[0] < rounds[0], again, (jnp.int32(1), best, ident)
    )
    return best.reshape(own), ident.reshape(own)


def solution(mesh):
    placed = P(AXES)
    return jax.shard_map(
        per_device,
        mesh=mesh,
        in_specs=(placed, placed, placed),
        out_specs=(placed, placed),
        check_vma=False,
    )
```

```python
import functools

import jax
import jax.numpy as jnp
from jax import lax
from jax.experimental import pallas as pl
from jax.experimental.pallas import tpu as pltpu
from jax.sharding import PartitionSpec as P

CELLS = 524288
VEHICLES = 1024
STEPS = 1024
AXES = ("gx", "gy")
LANES = 128
ROWS = 8
TILE = ROWS * LANES
BLOCK = LANES * LANES
CUT = 15
LOW = (1 << CUT) - 1
PITCH = ROWS + 1


def sub_iota():
    return lax.broadcasted_iota(jnp.int32, (ROWS, LANES), 0)


def lane_iota():
    return lax.broadcasted_iota(jnp.int32, (ROWS, LANES), 1)


def turned(regs):
    out = []
    for first in range(0, len(regs), 16):
        block = jnp.concatenate(regs[first : first + 16], axis=0).T
        out += [block[ROWS * i : ROWS * (i + 1)] for i in range(16)]
    return out


def place(bit, linear):
    if bit >= 14:
        return "v", bit - 10
    if linear:
        return ("l", bit) if bit < 7 else ("s", bit - 7) if bit < 10 else ("v", bit - 10)
    return ("s", bit) if bit < 3 else ("v", bit - 3) if bit < 7 else ("l", bit - 7)


def swapped(regs, ref):
    for g, x in enumerate(regs):
        ref[pl.ds(PITCH * g, ROWS), :] = x
    return [
        ref[pl.ds(PITCH * (g & ~7) + (g & 7), ROWS, stride=PITCH), :] for g in range(len(regs))
    ]


def exchange(keys, loads, low, high, more_keys=None, more_loads=None):
    more_keys = keys if more_keys is None else more_keys
    more_loads = loads if more_loads is None else more_loads
    a, b, p, q = keys[low], more_keys[high], loads[low], more_loads[high]
    larger = a > b
    keys[low], more_keys[high] = jnp.minimum(a, b), jnp.maximum(a, b)
    loads[low], more_loads[high] = jnp.where(larger, q, p), jnp.where(larger, p, q)


class Block:
    def __init__(self, load, index, linear, key_ref, load_ref):
        self.load, self.index = load, index
        self.spots = [place(bit, linear) for bit in range(14)]
        at = pl.ds(16 * PITCH * index, 16 * PITCH)
        self.refs = key_ref.at[at, :], load_ref.at[at, :]
        self.faced = None

    def moved(self, pairs, change):
        names = dict(pairs) | {b: a for a, b in pairs}
        self.spots = [names.get(spot, spot) for spot in self.spots]
        self.keys = change(self.keys, self.refs[0])
        self.loads = change(self.loads, self.refs[1])

    def turn(self):
        pairs = [(("s", b), ("l", b)) for b in range(3)]
        pairs += [(("v", b), ("l", b + 3)) for b in range(4)]
        self.moved(pairs, lambda regs, ref: turned(regs))

    def swap(self):
        self.moved([(("s", b), ("v", b)) for b in range(3)], swapped)

    def face(self, bit):
        odd, mask = [0] * 16, None
        for each in {self.faced, bit} - {None}:
            kind, at = self.spots[each] if each < 14 else ("h", each - 14)
            if kind == "h":
                odd = [x ^ (self.index >> at & 1) for x in odd]
            elif kind == "v":
                odd = [x ^ (g >> at & 1) for g, x in enumerate(odd)]
            else:
                index = sub_iota() if kind == "s" else lane_iota()
                one = -((index >> at) & 1)
                mask = one if mask is None else mask ^ one
        if mask is None:
            self.keys = [~x if o else x for x, o in zip(self.keys, odd)]
        else:
            masks = mask, ~mask
            self.keys = [x ^ masks[o] for x, o in zip(self.keys, odd)]
        self.faced = bit

    def levels(self, levels, bits):
        if self.load is not None:
            self.keys, self.loads = self.load()
            self.load = None
        for level in levels:
            if level < 15:
                self.face(level if level < bits else None)
            for bit in reversed(range(min(level, 14))):
                if self.spots[bit][0] == "l":
                    if level == bits and bit < 7 and self.spots[7][0] == "v":
                        self.swap()
                    yield
                    self.turn()
                if self.spots[bit][0] == "s":
                    self.swap()
                at = 1 << self.spots[bit][1]
                for low in range(16):
                    if not low & at:
                        exchange(self.keys, self.loads, low, low | at)


def run_all(takes):
    takes = list(takes)
    while takes:
        takes = [take for take in takes if next(take, takes) is not takes]


def sort_blocks(blocks, first):
    bits = 13 + len(blocks).bit_length()
    run_all(block.levels(range(first, min(bits, 14) + 1), bits) for block in blocks)
    for level in range(15, bits + 1):
        for block in blocks:
            block.face(level if level < bits else None)
        for bit in reversed(range(14, level)):
            for one in blocks:
                other = blocks[one.index | 1 << (bit - 14)]
                if other is not one:
                    for g in range(16):
                        exchange(one.keys, one.loads, g, g, other.keys, other.loads)
        run_all(block.levels([level], bits) for block in blocks)
    keys = sum((block.keys for block in blocks), [])
    return keys, sum((block.loads for block in blocks), [])


def lane_next(regs, fill):
    rolled = [pltpu.roll(x, LANES - 1, 1) for x in regs]
    rolled.append(jnp.full_like(rolled[0], fill))
    last = lane_iota() == LANES - 1
    return [jnp.where(last, rolled[h + 1], rolled[h]) for h in range(len(regs))]


def pull(regs, bit, linear):
    count = len(regs)
    blocks = count // 16
    kind, at = place(bit, linear)
    zero = jnp.zeros_like(regs[0])
    if kind == "s":
        step = 1 << at
        rolled = [pltpu.roll(x, ROWS - step, 0) for x in regs]
        stay = sub_iota() < ROWS - step
        if linear:
            over = rolled[1:] + [zero]
        else:
            wrap = lane_next([rolled[16 * h] for h in range(blocks)], 0)
            over = [rolled[g + 1] if (g + 1) % 16 else wrap[g // 16] for g in range(count)]
        return [jnp.where(stay, a, b) for a, b in zip(rolled, over)]
    step = 1 << at
    if linear or step >= 16:
        return regs[step:] + [zero] * step
    out = [None] * count
    for v in range(16):
        if v + step < 16:
            for h in range(blocks):
                out[16 * h + v] = regs[16 * h + v + step]
        else:
            wrap = lane_next([regs[16 * h + v + step - 16] for h in range(blocks)], 0)
            for h in range(blocks):
                out[16 * h + v] = wrap[h]
    return out


def pull_woven(regs, bit, linear):
    step = 1 << bit
    out = list(regs[step:]) + [None] * step
    bottom = sub_iota() == ROWS - 1
    for v in range(8 - step, 8):
        rolled = [pltpu.roll(x, ROWS - 1, 0) for x in regs[v + step - 8 :: 8]]
        wrap = lane_next(rolled[0::2], 0)
        for c, x in enumerate(rolled):
            out[8 * c + v] = jnp.where(bottom, wrap[c // 2] if c & 1 else rolled[c + 1], x)
    return out


def push(regs, bit, linear):
    assert len(regs) == 16
    kind, at = place(bit, linear)
    zero = jnp.zeros_like(regs[0])
    first = lane_iota() == 0

    def lane_last(x):
        return jnp.where(first, 0, pltpu.roll(x, 1, 1))

    step = 1 << at
    if kind == "s":
        rolled = [pltpu.roll(x, step, 0) for x in regs]
        over = [zero if linear else lane_last(rolled[15])] + rolled[:15]
        stay = sub_iota() >= step
        return [jnp.where(stay, a, b) for a, b in zip(rolled, over)]
    head = [zero] * step if linear else [lane_last(x) for x in regs[16 - step :]]
    return head + regs[: 16 - step]


def spread_row(x, row):
    return jnp.broadcast_to(x[row : row + 1], (ROWS, LANES))


def down_lanes(row):
    return turned([row] * 16)


def over_rows(regs, op):
    while len(regs) > 1:
        regs = [op(a, b) for a, b in zip(regs[0::2], regs[1::2])]
    x = regs[0]
    for step in (4, 2, 1):
        x = op(x, pltpu.roll(x, step, 0))
    return x


def run_max(cells, keys):
    count = len(cells)
    blocks = count // 16
    sub, lane = sub_iota(), lane_iota()
    keys = list(keys)

    def carry(g, cell, key, also=None):
        same = cells[g] == cell
        same = same if also is None else same & also
        keys[g] = jnp.where(same, jnp.maximum(keys[g], key), keys[g])

    for g in range(count):
        if g % 8:
            carry(g, cells[g - 1], keys[g - 1])
    ends = range(7, count, 8)
    final = [keys[g] for g in ends]
    last = [cells[g] for g in ends]

    def join(c, cell, key, also=None):
        same = last[c] == cell
        same = same if also is None else same & also
        final[c] = jnp.where(same, jnp.maximum(final[c], key), final[c])

    for step in (1, 2, 4):
        for c in range(len(last)):
            join(c, pltpu.roll(last[c], step, 0), pltpu.roll(final[c], step, 0), sub >= step)
    for c in range(1, len(last), 2):
        join(c, spread_row(last[c - 1], 7), spread_row(final[c - 1], 7))
    last_cell = [spread_row(x, 7) for x in last[1::2]]
    last_key = [spread_row(x, 7) for x in final[1::2]]
    rolled = [jnp.full((ROWS, LANES), -9, jnp.int32)] + [pltpu.roll(x, 1, 1) for x in last_cell]
    before = [jnp.where(lane == 0, rolled[h], rolled[h + 1]) for h in range(blocks)]
    cell_col = [down_lanes(x) for x in last_cell]
    key_col = [down_lanes(x) for x in last_key]
    for h in range(blocks):
        terms = []
        for source in range(h + 1):
            for v in range(16):
                match = cell_col[source][v] == before[h]
                if source == h:
                    match = match & (sub + ROWS * v < lane)
                terms.append(jnp.where(match, key_col[source][v], -1))
        while len(terms) & (len(terms) - 1):
            terms.append(terms[0])
        best = over_rows(terms, jnp.maximum)
        for c in (2 * h, 2 * h + 1):
            join(c, before[h], best)
            cell, key = before[h], best
            if c & 1:
                cell, key = spread_row(last[c - 1], 7), spread_row(final[c - 1], 7)
            cell = jnp.where(sub == 0, cell, pltpu.roll(last[c], 1, 0))
            key = jnp.where(sub == 0, key, pltpu.roll(final[c], 1, 0))
            for g in range(8 * c, 8 * c + 8):
                carry(g, cell, key)
    return keys


def run_ends(cells):
    count = len(cells)
    bottom = sub_iota() == ROWS - 1
    rolled = [pltpu.roll(x, ROWS - 1, 0) for x in cells[::8]]
    wrap = lane_next(rolled[::2], -9)
    out = []
    for g in range(count):
        c = g // 8
        if g % 8 < 7:
            after = cells[g + 1]
        else:
            after = jnp.where(bottom, wrap[c // 2] if c & 1 else rolled[c + 1], rolled[c])
        out.append(cells[g] != after)
    return out


def ranks(flags):
    count = len(flags)
    sub, lane = sub_iota(), lane_iota()
    out, total = [], jnp.zeros((ROWS, LANES), jnp.int32)
    for h in range(count // 16):
        starts, run = [], jnp.zeros((ROWS, LANES), jnp.int32)
        for c in (2 * h, 2 * h + 1):
            here = jnp.zeros((ROWS, LANES), jnp.int32)
            for g in range(8 * c, 8 * c + 8):
                out.append(here)
                here = here + flags[g]
            x = here
            for step in (1, 2, 4):
                x = x + jnp.where(sub >= step, pltpu.roll(x, step, 0), 0)
            starts.append(x - here + run)
            run = run + spread_row(x, 7)
        col = down_lanes(run)
        start = [jnp.where(sub + ROWS * v < lane, col[v], 0) for v in range(16)]
        start = over_rows(start, jnp.add) + total
        total = total + over_rows(col, jnp.add)
        starts = [x + start for x in starts]
        for g in range(16 * h, 16 * h + 16):
            out[g] = out[g] + starts[g // 8 % 2]
    return out, total


def positions(count, linear):
    sub, lane = sub_iota(), lane_iota()
    if linear:
        return [TILE * g + LANES * sub + lane for g in range(count)]
    weave = LANES * lane + ROWS * sub
    return [weave + (BLOCK * (g // 16) + 64 * (g // 8 % 2) + g % 8) for g in range(count)]


def travel(move, load, bit, linear, shift, empty):
    probe = 1 << (CUT + bit)
    new_move, new_load = shift(move, bit, linear), shift(load, bit, linear)
    for g in range(len(move)):
        arrives = (new_move[g] & probe) != 0
        old_move, old_load = move[g], load[g]
        if empty is not None:
            leaves = (old_move & probe) != 0
            old_move, old_load = jnp.where(leaves, 0, old_move), jnp.where(leaves, empty, old_load)
        new_move[g] = jnp.where(arrives, new_move[g], old_move)
        new_load[g] = jnp.where(arrives, new_load[g], old_load)
    return new_move, new_load


def compact(cells, keys, wanted, cell_ref, key_ref):
    count = len(cells)
    rank, total = ranks([jnp.where(w, 1, 0) for w in wanted])
    at = positions(count, False)
    move = [
        jnp.where(w, (i - r) << CUT | c, 0) for w, i, r, c in zip(wanted, at, rank, cells)
    ]
    for bit in range((count * TILE).bit_length() - 1):
        if bit == 3:
            move, keys = swapped(move, cell_ref), swapped(keys, key_ref)
        if bit == 7:
            move, keys = turned(move), turned(keys)
        move, keys = travel(move, keys, bit, bit >= 7, pull if bit >= 3 else pull_woven, None)
    return [x & LOW for x in move], keys, total


def owner_sizes(flags, cells, n, shift):
    sums = [jnp.zeros((ROWS, LANES), jnp.int32)] * (n // 4)
    for w, c in zip(flags, cells):
        group = jnp.where(w, c >> (shift + 2), -1)
        unit = jnp.left_shift(1, (c >> (shift - 3)) & 24)
        sums = [x + jnp.where(group == k, unit, 0) for k, x in enumerate(sums)]
    sizes = []
    for x in sums:
        pairs = []
        for part in (x & 0xFF00FF, (x >> 8) & 0xFF00FF):
            for step in (4, 2, 1):
                part = part + pltpu.roll(part, step, 0)
            pairs.append(part)
        for half in (0, 16):
            for part in pairs:
                row = (part >> half) & 0xFFFF
                sizes.append(jnp.sum(jnp.where(sub_iota() == 0, row, 0)))
    return sizes


def split_kernel(own, slots, chunk, round_ref, odd_ref, cell_in, vehicle_in, speed_in, out_ref, cell_ref, vehicle_ref, speed_ref, low_ref, high_ref, cell_pad, key_pad, in_sem):
    n = CELLS // own
    count = cell_ref.shape[0] // ROWS
    bits = (count * TILE).bit_length() - 1
    odd = odd_ref[0]
    arrays = ((cell_in, cell_ref), (vehicle_in, vehicle_ref), (speed_in, speed_ref))
    copies = []
    for h in range(count // 16):
        part = pl.ds(LANES * h, LANES)
        copies.append(
            [
                pltpu.make_async_copy(x.at[part, :], y.at[part, :], in_sem.at[h, k])
                for k, (x, y) in enumerate(arrays)
            ]
        )
        for copy in copies[h]:
            copy.start()
    blocks = []
    for h in range(count // 16):
        for copy in copies[h]:
            copy.wait()
        some_cells, some_keys = [], []
        for g in range(16 * h, 16 * h + 16):
            at = pl.ds(ROWS * g, ROWS)
            cell = cell_ref[at, :]
            some_cells.append(jnp.where(odd == 1, CELLS - 1 - cell, cell))
            level = (speed_ref[at, :] * float(STEPS)).astype(jnp.int32)
            some_keys.append(level * VEHICLES + (VEHICLES - 1 - vehicle_ref[at, :]))
        block = Block(lambda: (some_cells, some_keys), h, False, cell_pad, key_pad)
        run_all([block.levels(range(1, 8), bits)])
        blocks.append(block)
    cells, keys = sort_blocks(blocks, 8)
    keys = run_max(cells, keys)
    ends = run_ends(cells)
    shift = own.bit_length() - 1
    sizes = owner_sizes(ends, cells, n, shift)
    high = [k | (c >> CUT) << 27 for k, c in zip(keys, cells)]
    low, high, _ = compact([c & LOW for c in cells], high, ends, cell_pad, key_pad)
    for g in range(count):
        at = pl.ds(ROWS * g, ROWS)
        low_ref[at, :] = low[g]
        high_ref[at, :] = high[g]
    low_ref[pl.ds(ROWS * count, ROWS), :] = jnp.zeros((ROWS, LANES), jnp.int32)
    high_ref[pl.ds(ROWS * count, ROWS), :] = jnp.zeros((ROWS, LANES), jnp.int32)
    most = functools.reduce(jnp.maximum, sizes)
    sub, lane = sub_iota(), lane_iota()
    skip = round_ref[0] * (slots * LANES)
    base = jnp.int32(0)
    for o in range(n):
        start = base + skip
        valid = sub * LANES + lane < sizes[o] - skip
        start = jnp.minimum(start, count * TILE)
        base = base + sizes[o]
        row, off = start >> 7, start & 127

        def window(ref):
            x = pltpu.roll(ref[pl.ds(row, ROWS), :], (LANES - off) & 127, 1)
            return jnp.where(lane < LANES - off, x, pltpu.roll(x, ROWS - 1, 0))

        low_w, high_w = window(low_ref), window(high_ref)
        cell = jnp.where(valid, low_w & (own - 1), own).astype(jnp.float32)
        level = (high_w & ((1 << 27) - 1)) >> 10
        speed = level.astype(jnp.float32) * (1.0 / STEPS)
        ident = (~high_w & (VEHICLES - 1)).astype(jnp.float32)
        target = pl.multiple_of(jnp.where(odd == 1, n - 1 - o, o) * chunk, chunk)
        for w, x in enumerate((cell, speed, ident)):
            out_ref[pl.ds(target + w * slots, slots), :] = x[:slots]
        tail = chunk - 3 * slots
        fill = jnp.full((tail, LANES), most.astype(jnp.float32))
        out_ref[pl.ds(target + 3 * slots, tail), :] = fill


def join_kernel(own, n, slots, chunk, in_ref, speed_ref, ident_ref, rounds_ref, cell_pad, key_pad):
    sub = sub_iota()
    per = ROWS // run_rows(slots)

    def load(h):
        cells, keys = [], []
        late = jnp.where(blocks[h - 1].loads[15] > 1 << 30, 1, 0) if h else 0
        for g in range(16 * h, 16 * h + 16):
            if per == 1:
                part = [in_ref[pl.ds(chunk * g + w * slots, slots), :] for w in range(3)]
                pad = jnp.zeros((ROWS - slots, LANES), jnp.float32)
                part = [jnp.concatenate([x, pad], axis=0) for x in part]
                cell = jnp.where(sub < slots, part[0].astype(jnp.int32), own)
                cell = own - 1 - cell if g & 1 else cell
            else:
                part = [
                    in_ref[pl.ds(chunk * per * g + w, ROWS, stride=chunk), :] for w in range(3)
                ]
                cell = part[0].astype(jnp.int32)
                cell = jnp.where(sub & 1 == 1, own - 1 - cell, cell)
            level = (part[1] * float(STEPS)).astype(jnp.int32)
            cells.append(cell + late)
            keys.append(level * VEHICLES + (VEHICLES - 1 - part[2].astype(jnp.int32)))
        return cells, keys

    most = jnp.zeros((ROWS, LANES), jnp.float32)
    for source in range(n):
        most = jnp.maximum(most, in_ref[pl.ds(chunk * (source + 1) - ROWS, ROWS), :])
    most = jnp.max(jnp.where(sub == ROWS - 1, most, 0.0)).astype(jnp.int32)
    rounds_ref[0] = lax.div(most + (slots * LANES - 1), jnp.int32(slots * LANES))
    first = (run_rows(slots) * LANES).bit_length()
    blocks = [
        Block(functools.partial(load, h), h, True, cell_pad, key_pad) for h in range(n // per // 16)
    ]
    cells, keys = sort_blocks(blocks, first)
    keys = run_max(cells, keys)
    ends = [w & (c >= 0) & (c < own) for w, c in zip(run_ends(cells), cells)]
    cells, keys, total = compact(cells, keys, ends, cell_pad, key_pad)
    keep = max(own // TILE, 1)
    at = positions(16, True)
    move = [jnp.where(i < total, (c - i) << CUT, 0) for i, c in zip(at, cells)]
    keys = [jnp.where(i < total, k, -1) for i, k in zip(at, keys)]
    linear = True
    for bit in reversed(range(own.bit_length() - 1)):
        if bit == 6:
            move, keys, linear = turned(move), turned(keys), False
        move, keys = travel(move, keys, bit, linear, push, -1)
    keys = turned(keys)
    for g in range(keep):
        key = keys[g]
        at = pl.ds(ROWS * g, ROWS)
        speed = (key >> 10).astype(jnp.float32) * (1.0 / STEPS)
        speed_ref[at, :] = jnp.where(key >= 0, speed, -1.0)
        ident_ref[at, :] = jnp.where(key >= 0, VEHICLES - 1 - (key & (VEHICLES - 1)), -1)


def run_rows(slots):
    return 1 << (slots - 1).bit_length()


def pads(rows):
    return [pltpu.VMEM((rows // ROWS * PITCH, LANES), jnp.int32)] * 2


def per_device(cell, vehicle, speed):
    n = lax.axis_size(AXES)
    own = CELLS // n
    events = cell.shape[0]
    slots = max(1, (5 * events // n) // (8 * LANES))
    chunk = -(-(3 * slots + 1) // ROWS) * ROWS
    rows = events // LANES
    smem = pl.BlockSpec(memory_space=pltpu.SMEM)
    vmem = pl.BlockSpec(memory_space=pltpu.VMEM)
    hbm = pl.BlockSpec(memory_space=pl.ANY)
    params = pltpu.CompilerParams(vmem_limit_bytes=16 << 20)
    table = (own // LANES, LANES)
    odd = (lax.axis_index(AXES) & 1).reshape(1)
    inputs = [x.reshape(rows, LANES) for x in (cell, vehicle, speed)]

    split = pl.pallas_call(
        functools.partial(split_kernel, own, slots, chunk),
        out_shape=pltpu.VMEM((n * chunk, LANES), jnp.float32),
        in_specs=[smem, smem, hbm, hbm, hbm],
        out_specs=vmem,
        scratch_shapes=[
            pltpu.VMEM((rows, LANES), jnp.int32),
            pltpu.VMEM((rows, LANES), jnp.int32),
            pltpu.VMEM((rows, LANES), jnp.float32),
            pltpu.VMEM((rows + ROWS, LANES), jnp.int32),
            pltpu.VMEM((rows + ROWS, LANES), jnp.int32),
        ]
        + pads(rows)
        + [pltpu.SemaphoreType.DMA((rows // LANES, 3))],
        compiler_params=params,
        name="split",
    )
    join = pl.pallas_call(
        functools.partial(join_kernel, own, n, slots, chunk),
        out_shape=(
            jax.ShapeDtypeStruct(table, jnp.float32),
            jax.ShapeDtypeStruct(table, jnp.int32),
            jax.ShapeDtypeStruct((1,), jnp.int32),
        ),
        in_specs=[vmem],
        out_specs=(vmem, vmem, smem),
        scratch_shapes=pads(n * run_rows(slots)),
        compiler_params=params,
        name="join",
    )

    def one_round(index):
        sent = split(index.reshape(1), odd, *inputs)
        got = lax.all_to_all(sent.reshape(n, chunk, LANES), AXES, 0, 0, tiled=True)
        return join(got.reshape(n * chunk, LANES))

    best, ident, rounds = one_round(jnp.int32(0))

    def again(state):
        index, best, ident = state
        more, other, _ = one_round(index)
        ident = jnp.where(
            more > best, other, jnp.where(more < best, ident, jnp.minimum(ident, other))
        )
        return index + 1, jnp.maximum(best, more), ident

    def rest(best, ident):
        state = (jnp.int32(1), best, ident)
        return lax.while_loop(lambda state: state[0] < rounds[0], again, state)[1:]

    best, ident = lax.cond(rounds[0] > 1, rest, lambda *kept: kept, best, ident)
    return best.reshape(own), ident.reshape(own)


def solution(mesh):
    placed = P(AXES)
    return jax.shard_map(
        per_device,
        mesh=mesh,
        in_specs=(placed, placed, placed),
        out_specs=(placed, placed),
        check_vma=False,
    )
```

```python
import functools

import jax
import jax.numpy as jnp
from jax import lax
from jax.experimental import pallas as pl
from jax.experimental.pallas import tpu as pltpu
from jax.sharding import PartitionSpec as P

CELLS = 524288
VEHICLES = 1024
STEPS = 1024
AXES = ("gx", "gy")
LANES = 128
ROWS = 8
TILE = ROWS * LANES
BLOCK = LANES * LANES
CUT = 15
LOW = (1 << CUT) - 1
PITCH = ROWS + 1


def sub_iota():
    return lax.broadcasted_iota(jnp.int32, (ROWS, LANES), 0)


def lane_iota():
    return lax.broadcasted_iota(jnp.int32, (ROWS, LANES), 1)


def turned(regs):
    out = []
    for first in range(0, len(regs), 16):
        block = jnp.concatenate(regs[first : first + 16], axis=0).T
        out += [block[ROWS * i : ROWS * (i + 1)] for i in range(16)]
    return out


def place(bit, linear):
    if bit >= 14:
        return "v", bit - 10
    if linear:
        return ("l", bit) if bit < 7 else ("s", bit - 7) if bit < 10 else ("v", bit - 10)
    return ("s", bit) if bit < 3 else ("v", bit - 3) if bit < 7 else ("l", bit - 7)


def swapped(regs, ref):
    for g, x in enumerate(regs):
        ref[pl.ds(PITCH * g, ROWS), :] = x
    return [
        ref[pl.ds(PITCH * (g & ~7) + (g & 7), ROWS, stride=PITCH), :] for g in range(len(regs))
    ]


def exchange(keys, loads, low, high, more_keys=None, more_loads=None):
    more_keys = keys if more_keys is None else more_keys
    more_loads = loads if more_loads is None else more_loads
    a, b, p, q = keys[low], more_keys[high], loads[low], more_loads[high]
    larger = a > b
    keys[low], more_keys[high] = jnp.minimum(a, b), jnp.maximum(a, b)
    loads[low], more_loads[high] = jnp.where(larger, q, p), jnp.where(larger, p, q)


class Block:
    def __init__(self, load, index, linear, key_ref, load_ref):
        self.load, self.index = load, index
        self.spots = [place(bit, linear) for bit in range(14)]
        at = pl.ds(16 * PITCH * index, 16 * PITCH)
        self.refs = key_ref.at[at, :], load_ref.at[at, :]
        self.faced = None

    def moved(self, pairs, change):
        names = dict(pairs) | {b: a for a, b in pairs}
        self.spots = [names.get(spot, spot) for spot in self.spots]
        self.keys = change(self.keys, self.refs[0])
        self.loads = change(self.loads, self.refs[1])

    def turn(self):
        pairs = [(("s", b), ("l", b)) for b in range(3)]
        pairs += [(("v", b), ("l", b + 3)) for b in range(4)]
        self.moved(pairs, lambda regs, ref: turned(regs))

    def swap(self):
        self.moved([(("s", b), ("v", b)) for b in range(3)], swapped)

    def face(self, bit):
        odd, mask = [0] * 16, None
        for each in {self.faced, bit} - {None}:
            kind, at = self.spots[each] if each < 14 else ("h", each - 14)
            if kind == "h":
                odd = [x ^ (self.index >> at & 1) for x in odd]
            elif kind == "v":
                odd = [x ^ (g >> at & 1) for g, x in enumerate(odd)]
            else:
                index = sub_iota() if kind == "s" else lane_iota()
                one = -((index >> at) & 1)
                mask = one if mask is None else mask ^ one
        if mask is None:
            self.keys = [~x if o else x for x, o in zip(self.keys, odd)]
        else:
            masks = mask, ~mask
            self.keys = [x ^ masks[o] for x, o in zip(self.keys, odd)]
        self.faced = bit

    def levels(self, levels, bits):
        if self.load is not None:
            self.keys, self.loads = self.load()
            self.load = None
        if levels[0] >= 15 and self.index:
            late = jnp.where(self.before.loads[15] > 1 << 30, 1, 0)
            self.keys = [x + late for x in self.keys]
        for level in levels:
            if level < 15:
                self.face(level if level < bits else None)
            for bit in reversed(range(min(level, 14))):
                if self.spots[bit][0] == "l":
                    if level == bits and bit < 7 and self.spots[7][0] == "v":
                        self.swap()
                    yield
                    self.turn()
                if self.spots[bit][0] == "s":
                    self.swap()
                at = 1 << self.spots[bit][1]
                for low in range(16):
                    if not low & at:
                        exchange(self.keys, self.loads, low, low | at)


def run_all(takes):
    takes = list(takes)
    while takes:
        takes = [take for take in takes if next(take, takes) is not takes]


def sort_blocks(blocks, first):
    bits = 13 + len(blocks).bit_length()
    run_all(block.levels(range(first, min(bits, 14) + 1), bits) for block in blocks)
    for level in range(15, bits + 1):
        for block in blocks:
            block.face(level if level < bits else None)
        for bit in reversed(range(14, level)):
            for one in blocks:
                other = blocks[one.index | 1 << (bit - 14)]
                if other is not one:
                    for g in range(16):
                        exchange(one.keys, one.loads, g, g, other.keys, other.loads)
        for block in blocks[1:]:
            block.before = blocks[block.index - 1]
        run_all(block.levels([level], bits) for block in blocks)
    keys = sum((block.keys for block in blocks), [])
    return keys, sum((block.loads for block in blocks), [])


def lane_next(regs, fill):
    rolled = [pltpu.roll(x, LANES - 1, 1) for x in regs]
    rolled.append(jnp.full_like(rolled[0], fill))
    last = lane_iota() == LANES - 1
    return [jnp.where(last, rolled[h + 1], rolled[h]) for h in range(len(regs))]


def pull(regs, bit, linear):
    count = len(regs)
    blocks = count // 16
    kind, at = place(bit, linear)
    zero = jnp.zeros_like(regs[0])
    if kind == "s":
        step = 1 << at
        rolled = [pltpu.roll(x, ROWS - step, 0) for x in regs]
        stay = sub_iota() < ROWS - step
        if linear:
            over = rolled[1:] + [zero]
        else:
            wrap = lane_next([rolled[16 * h] for h in range(blocks)], 0)
            over = [rolled[g + 1] if (g + 1) % 16 else wrap[g // 16] for g in range(count)]
        return [jnp.where(stay, a, b) for a, b in zip(rolled, over)]
    step = 1 << at
    if linear or step >= 16:
        return regs[step:] + [zero] * step
    out = [None] * count
    for v in range(16):
        if v + step < 16:
            for h in range(blocks):
                out[16 * h + v] = regs[16 * h + v + step]
        else:
            wrap = lane_next([regs[16 * h + v + step - 16] for h in range(blocks)], 0)
            for h in range(blocks):
                out[16 * h + v] = wrap[h]
    return out


def pull_woven(regs, bit, linear):
    step = 1 << bit
    out = list(regs[step:]) + [None] * step
    bottom = sub_iota() == ROWS - 1
    for v in range(8 - step, 8):
        rolled = [pltpu.roll(x, ROWS - 1, 0) for x in regs[v + step - 8 :: 8]]
        wrap = lane_next(rolled[0::2], 0)
        for c, x in enumerate(rolled):
            out[8 * c + v] = jnp.where(bottom, wrap[c // 2] if c & 1 else rolled[c + 1], x)
    return out


def push(regs, bit, linear):
    assert len(regs) == 16
    kind, at = place(bit, linear)
    zero = jnp.zeros_like(regs[0])
    first = lane_iota() == 0

    def lane_last(x):
        return jnp.where(first, 0, pltpu.roll(x, 1, 1))

    step = 1 << at
    if kind == "s":
        rolled = [pltpu.roll(x, step, 0) for x in regs]
        over = [zero if linear else lane_last(rolled[15])] + rolled[:15]
        stay = sub_iota() >= step
        return [jnp.where(stay, a, b) for a, b in zip(rolled, over)]
    head = [zero] * step if linear else [lane_last(x) for x in regs[16 - step :]]
    return head + regs[: 16 - step]


def spread_row(x, row):
    return jnp.broadcast_to(x[row : row + 1], (ROWS, LANES))


def down_lanes(row):
    return turned([row] * 16)


def over_rows(regs, op):
    while len(regs) > 1:
        regs = [op(a, b) for a, b in zip(regs[0::2], regs[1::2])]
    x = regs[0]
    for step in (4, 2, 1):
        x = op(x, pltpu.roll(x, step, 0))
    return x


def run_max(cells, keys):
    count = len(cells)
    blocks = count // 16
    sub, lane = sub_iota(), lane_iota()
    keys = list(keys)

    def carry(g, cell, key, also=None):
        same = cells[g] == cell
        same = same if also is None else same & also
        keys[g] = jnp.where(same, jnp.maximum(keys[g], key), keys[g])

    for g in range(count):
        if g % 8:
            carry(g, cells[g - 1], keys[g - 1])
    ends = range(7, count, 8)
    final = [keys[g] for g in ends]
    last = [cells[g] for g in ends]

    def join(c, cell, key, also=None):
        same = last[c] == cell
        same = same if also is None else same & also
        final[c] = jnp.where(same, jnp.maximum(final[c], key), final[c])

    for step in (1, 2, 4):
        for c in range(len(last)):
            join(c, pltpu.roll(last[c], step, 0), pltpu.roll(final[c], step, 0), sub >= step)
    for c in range(1, len(last), 2):
        join(c, spread_row(last[c - 1], 7), spread_row(final[c - 1], 7))
    last_cell = [spread_row(x, 7) for x in last[1::2]]
    last_key = [spread_row(x, 7) for x in final[1::2]]
    rolled = [jnp.full((ROWS, LANES), -9, jnp.int32)] + [pltpu.roll(x, 1, 1) for x in last_cell]
    before = [jnp.where(lane == 0, rolled[h], rolled[h + 1]) for h in range(blocks)]
    cell_col = [down_lanes(x) for x in last_cell]
    key_col = [down_lanes(x) for x in last_key]
    for h in range(blocks):
        terms = []
        for source in range(h + 1):
            for v in range(16):
                match = cell_col[source][v] == before[h]
                if source == h:
                    match = match & (sub + ROWS * v < lane)
                terms.append(jnp.where(match, key_col[source][v], -1))
        while len(terms) & (len(terms) - 1):
            terms.append(terms[0])
        best = over_rows(terms, jnp.maximum)
        for c in (2 * h, 2 * h + 1):
            join(c, before[h], best)
            cell, key = before[h], best
            if c & 1:
                cell, key = spread_row(last[c - 1], 7), spread_row(final[c - 1], 7)
            cell = jnp.where(sub == 0, cell, pltpu.roll(last[c], 1, 0))
            key = jnp.where(sub == 0, key, pltpu.roll(final[c], 1, 0))
            for g in range(8 * c, 8 * c + 8):
                carry(g, cell, key)
    return keys


def run_ends(cells):
    count = len(cells)
    bottom = sub_iota() == ROWS - 1
    rolled = [pltpu.roll(x, ROWS - 1, 0) for x in cells[::8]]
    wrap = lane_next(rolled[::2], -9)
    out = []
    for g in range(count):
        c = g // 8
        if g % 8 < 7:
            after = cells[g + 1]
        else:
            after = jnp.where(bottom, wrap[c // 2] if c & 1 else rolled[c + 1], rolled[c])
        out.append(cells[g] != after)
    return out


def ranks(flags):
    count = len(flags)
    sub, lane = sub_iota(), lane_iota()
    out, total = [], jnp.zeros((ROWS, LANES), jnp.int32)
    for h in range(count // 16):
        starts, run = [], jnp.zeros((ROWS, LANES), jnp.int32)
        for c in (2 * h, 2 * h + 1):
            here = jnp.zeros((ROWS, LANES), jnp.int32)
            for g in range(8 * c, 8 * c + 8):
                out.append(here)
                here = here + flags[g]
            x = here
            for step in (1, 2, 4):
                x = x + jnp.where(sub >= step, pltpu.roll(x, step, 0), 0)
            starts.append(x - here + run)
            run = run + spread_row(x, 7)
        col = down_lanes(run)
        start = [jnp.where(sub + ROWS * v < lane, col[v], 0) for v in range(16)]
        start = over_rows(start, jnp.add) + total
        total = total + over_rows(col, jnp.add)
        starts = [x + start for x in starts]
        for g in range(16 * h, 16 * h + 16):
            out[g] = out[g] + starts[g // 8 % 2]
    return out, total


def positions(count, linear):
    sub, lane = sub_iota(), lane_iota()
    if linear:
        return [TILE * g + LANES * sub + lane for g in range(count)]
    weave = LANES * lane + ROWS * sub
    return [weave + (BLOCK * (g // 16) + 64 * (g // 8 % 2) + g % 8) for g in range(count)]


def travel(move, load, bit, linear, shift, empty):
    probe = 1 << (CUT + bit)
    new_move, new_load = shift(move, bit, linear), shift(load, bit, linear)
    for g in range(len(move)):
        arrives = (new_move[g] & probe) != 0
        old_move, old_load = move[g], load[g]
        if empty is not None:
            leaves = (old_move & probe) != 0
            old_move, old_load = jnp.where(leaves, 0, old_move), jnp.where(leaves, empty, old_load)
        new_move[g] = jnp.where(arrives, new_move[g], old_move)
        new_load[g] = jnp.where(arrives, new_load[g], old_load)
    return new_move, new_load


def compact(cells, keys, wanted, cell_ref, key_ref):
    count = len(cells)
    rank, total = ranks([jnp.where(w, 1, 0) for w in wanted])
    at = positions(count, False)
    move = [
        jnp.where(w, (i - r) << CUT | c, 0) for w, i, r, c in zip(wanted, at, rank, cells)
    ]
    for bit in range((count * TILE).bit_length() - 1):
        if bit == 3:
            move, keys = swapped(move, cell_ref), swapped(keys, key_ref)
        if bit == 7:
            move, keys = turned(move), turned(keys)
        move, keys = travel(move, keys, bit, bit >= 7, pull if bit >= 3 else pull_woven, None)
    return [x & LOW for x in move], keys, total


def owner_sizes(flags, cells, n, shift):
    sums = [jnp.zeros((ROWS, LANES), jnp.int32)] * (n // 4)
    for w, c in zip(flags, cells):
        group = jnp.where(w, c >> (shift + 2), -1)
        unit = jnp.left_shift(1, (c >> (shift - 3)) & 24)
        sums = [x + jnp.where(group == k, unit, 0) for k, x in enumerate(sums)]
    sizes = []
    for x in sums:
        pairs = []
        for part in (x & 0xFF00FF, (x >> 8) & 0xFF00FF):
            for step in (4, 2, 1):
                part = part + pltpu.roll(part, step, 0)
            pairs.append(part)
        for half in (0, 16):
            for part in pairs:
                row = (part >> half) & 0xFFFF
                sizes.append(jnp.sum(jnp.where(sub_iota() == 0, row, 0)))
    return sizes


def split_kernel(own, slots, chunk, round_ref, odd_ref, cell_in, vehicle_in, speed_in, out_ref, cell_ref, vehicle_ref, speed_ref, low_ref, high_ref, cell_pad, key_pad, in_sem):
    n = CELLS // own
    count = cell_ref.shape[0] // ROWS
    bits = (count * TILE).bit_length() - 1
    odd = odd_ref[0]
    arrays = ((cell_in, cell_ref), (vehicle_in, vehicle_ref), (speed_in, speed_ref))
    copies = []
    for h in range(count // 16):
        part = pl.ds(LANES * h, LANES)
        copies.append(
            [
                pltpu.make_async_copy(x.at[part, :], y.at[part, :], in_sem.at[h, k])
                for k, (x, y) in enumerate(arrays)
            ]
        )
        for copy in copies[h]:
            copy.start()
    blocks = []
    for h in range(count // 16):
        for copy in copies[h]:
            copy.wait()
        some_cells, some_keys = [], []
        for g in range(16 * h, 16 * h + 16):
            at = pl.ds(ROWS * g, ROWS)
            cell = cell_ref[at, :]
            some_cells.append(jnp.where(odd == 1, CELLS - 1 - cell, cell))
            level = (speed_ref[at, :] * float(STEPS)).astype(jnp.int32)
            some_keys.append(level * VEHICLES + (VEHICLES - 1 - vehicle_ref[at, :]))
        block = Block(lambda: (some_cells, some_keys), h, False, cell_pad, key_pad)
        run_all([block.levels(range(1, 8), bits)])
        blocks.append(block)
    cells, keys = sort_blocks(blocks, 8)
    keys = run_max(cells, keys)
    ends = run_ends(cells)
    shift = own.bit_length() - 1
    sizes = owner_sizes(ends, cells, n, shift)
    high = [k | (c >> CUT) << 27 for k, c in zip(keys, cells)]
    low, high, _ = compact([c & LOW for c in cells], high, ends, cell_pad, key_pad)
    for g in range(count):
        at = pl.ds(ROWS * g, ROWS)
        low_ref[at, :] = low[g]
        high_ref[at, :] = high[g]
    low_ref[pl.ds(ROWS * count, ROWS), :] = jnp.zeros((ROWS, LANES), jnp.int32)
    high_ref[pl.ds(ROWS * count, ROWS), :] = jnp.zeros((ROWS, LANES), jnp.int32)
    most = functools.reduce(jnp.maximum, sizes)
    sub, lane = sub_iota(), lane_iota()
    skip = round_ref[0] * (slots * LANES)
    base = jnp.int32(0)
    for o in range(n):
        start = base + skip
        valid = sub * LANES + lane < sizes[o] - skip
        start = jnp.minimum(start, count * TILE)
        base = base + sizes[o]
        row, off = start >> 7, start & 127

        def window(ref):
            x = pltpu.roll(ref[pl.ds(row, ROWS), :], (LANES - off) & 127, 1)
            return jnp.where(lane < LANES - off, x, pltpu.roll(x, ROWS - 1, 0))

        low_w, high_w = window(low_ref), window(high_ref)
        cell = jnp.where(valid, low_w & (own - 1), own).astype(jnp.float32)
        level = (high_w & ((1 << 27) - 1)) >> 10
        speed = level.astype(jnp.float32) * (1.0 / STEPS)
        ident = (~high_w & (VEHICLES - 1)).astype(jnp.float32)
        target = pl.multiple_of(jnp.where(odd == 1, n - 1 - o, o) * chunk, chunk)
        for w, x in enumerate((cell, speed, ident)):
            out_ref[pl.ds(target + w * slots, slots), :] = x[:slots]
        tail = chunk - 3 * slots
        fill = jnp.full((tail, LANES), most.astype(jnp.float32))
        out_ref[pl.ds(target + 3 * slots, tail), :] = fill


def join_kernel(own, n, slots, chunk, in_ref, speed_ref, ident_ref, rounds_ref, cell_pad, key_pad):
    sub = sub_iota()
    per = ROWS // run_rows(slots)

    def load(h):
        cells, keys = [], []
        late = jnp.where(blocks[h - 1].loads[15] > 1 << 30, 1, 0) if h else 0
        for g in range(16 * h, 16 * h + 16):
            if per == 1:
                part = [in_ref[pl.ds(chunk * g + w * slots, slots), :] for w in range(3)]
                pad = jnp.zeros((ROWS - slots, LANES), jnp.float32)
                part = [jnp.concatenate([x, pad], axis=0) for x in part]
                cell = jnp.where(sub < slots, part[0].astype(jnp.int32), own)
                cell = own - 1 - cell if g & 1 else cell
            else:
                part = [
                    in_ref[pl.ds(chunk * per * g + w, ROWS, stride=chunk), :] for w in range(3)
                ]
                cell = part[0].astype(jnp.int32)
                cell = jnp.where(sub & 1 == 1, own - 1 - cell, cell)
            level = (part[1] * float(STEPS)).astype(jnp.int32)
            cells.append(cell + late)
            keys.append(level * VEHICLES + (VEHICLES - 1 - part[2].astype(jnp.int32)))
        return cells, keys

    most = jnp.zeros((ROWS, LANES), jnp.float32)
    for source in range(n):
        most = jnp.maximum(most, in_ref[pl.ds(chunk * (source + 1) - ROWS, ROWS), :])
    most = jnp.max(jnp.where(sub == ROWS - 1, most, 0.0)).astype(jnp.int32)
    rounds_ref[0] = lax.div(most + (slots * LANES - 1), jnp.int32(slots * LANES))
    first = (run_rows(slots) * LANES).bit_length()
    blocks = [
        Block(functools.partial(load, h), h, True, cell_pad, key_pad) for h in range(n // per // 16)
    ]
    cells, keys = sort_blocks(blocks, first)
    keys = run_max(cells, keys)
    ends = [w & (c >= 0) & (c < own) for w, c in zip(run_ends(cells), cells)]
    cells, keys, total = compact(cells, keys, ends, cell_pad, key_pad)
    keep = max(own // TILE, 1)
    at = positions(16, True)
    move = [jnp.where(i < total, (c - i) << CUT, 0) for i, c in zip(at, cells)]
    keys = [jnp.where(i < total, k, -1) for i, k in zip(at, keys)]
    linear = True
    for bit in reversed(range(own.bit_length() - 1)):
        if bit == 6:
            move, keys, linear = turned(move), turned(keys), False
        move, keys = travel(move, keys, bit, linear, push, -1)
    keys = turned(keys)
    for g in range(keep):
        key = keys[g]
        at = pl.ds(ROWS * g, ROWS)
        speed = (key >> 10).astype(jnp.float32) * (1.0 / STEPS)
        speed_ref[at, :] = jnp.where(key >= 0, speed, -1.0)
        ident_ref[at, :] = jnp.where(key >= 0, VEHICLES - 1 - (key & (VEHICLES - 1)), -1)


def run_rows(slots):
    return 1 << (slots - 1).bit_length()


def pads(rows):
    return [pltpu.VMEM((rows // ROWS * PITCH, LANES), jnp.int32)] * 2


def per_device(cell, vehicle, speed):
    n = lax.axis_size(AXES)
    own = CELLS // n
    events = cell.shape[0]
    slots = max(1, (5 * events // n) // (8 * LANES))
    chunk = -(-(3 * slots + 1) // ROWS) * ROWS
    rows = events // LANES
    smem = pl.BlockSpec(memory_space=pltpu.SMEM)
    vmem = pl.BlockSpec(memory_space=pltpu.VMEM)
    hbm = pl.BlockSpec(memory_space=pl.ANY)
    params = pltpu.CompilerParams(vmem_limit_bytes=16 << 20)
    table = (own // LANES, LANES)
    odd = (lax.axis_index(AXES) & 1).reshape(1)
    inputs = [x.reshape(rows, LANES) for x in (cell, vehicle, speed)]

    split = pl.pallas_call(
        functools.partial(split_kernel, own, slots, chunk),
        out_shape=pltpu.VMEM((n * chunk, LANES), jnp.float32),
        in_specs=[smem, smem, hbm, hbm, hbm],
        out_specs=vmem,
        scratch_shapes=[
            pltpu.VMEM((rows, LANES), jnp.int32),
            pltpu.VMEM((rows, LANES), jnp.int32),
            pltpu.VMEM((rows, LANES), jnp.float32),
            pltpu.VMEM((rows + ROWS, LANES), jnp.int32),
            pltpu.VMEM((rows + ROWS, LANES), jnp.int32),
        ]
        + pads(rows)
        + [pltpu.SemaphoreType.DMA((rows // LANES, 3))],
        compiler_params=params,
        name="split",
    )
    join = pl.pallas_call(
        functools.partial(join_kernel, own, n, slots, chunk),
        out_shape=(
            jax.ShapeDtypeStruct(table, jnp.float32),
            jax.ShapeDtypeStruct(table, jnp.int32),
            jax.ShapeDtypeStruct((1,), jnp.int32),
        ),
        in_specs=[vmem],
        out_specs=(vmem, vmem, smem),
        scratch_shapes=pads(n * run_rows(slots)),
        compiler_params=params,
        name="join",
    )

    def one_round(index):
        sent = split(index.reshape(1), odd, *inputs)
        got = lax.all_to_all(sent.reshape(n, chunk, LANES), AXES, 0, 0, tiled=True)
        return join(got.reshape(n * chunk, LANES))

    best, ident, rounds = one_round(jnp.int32(0))

    def again(state):
        index, best, ident = state
        more, other, _ = one_round(index)
        ident = jnp.where(
            more > best, other, jnp.where(more < best, ident, jnp.minimum(ident, other))
        )
        return index + 1, jnp.maximum(best, more), ident

    def rest(best, ident):
        state = (jnp.int32(1), best, ident)
        return lax.while_loop(lambda state: state[0] < rounds[0], again, state)[1:]

    best, ident = lax.cond(rounds[0] > 1, rest, lambda *kept: kept, best, ident)
    return best.reshape(own), ident.reshape(own)


def solution(mesh):
    placed = P(AXES)
    return jax.shard_map(
        per_device,
        mesh=mesh,
        in_specs=(placed, placed, placed),
        out_specs=(placed, placed),
        check_vma=False,
    )
```
